32 devices in a mesh: ka: 16 (over z, y, x), occ: 2 (over core).
Axes of the slice: x: 2, y: 2, z: 4, core: 2. Of those that a mesh axis runs over, the one named last changes fastest.
Arguments:
- factors: bfloat16 [32, 2, 192, 2, 768], P('ka'), may hold values from -0.23925781 to 0.23925781
- occupied_energy: float32 [2], replicated, may hold values from -2 to -0.5
- virtual_energy: bfloat16 [32, 192], P('ka'), may hold values from 0.5 to 3
- conserve: int32 [32, 2], P('ka'), may hold values from 0 to 31, as said below
- pair_lists: int32 [2, 4, 2], P(None, 'occ'), may hold values from 0 to 1, as said below
Outputs:
- density: float32 [32, 192, 2, 192], P('ka', 'occ')
The draws below stay inside these ranges and needn't reach their ends.
Inputs may be any that keep to these rules, and one draw needn't show every extreme that they name: For a momentum ka among the 2 momenta of block d (momenta d * 2 to d * 2 + 1), (32 - conserve[ka, r]) mod 32 lies in block (d - r - 1) mod 16; the 2 momenta of one block name different momenta in each round. `pair_lists`: each entry is an ordered pair (i, j) of occupied orbitals; every round begins with the pairs (0, 0) and (1, 1); within a round no ordered pair repeats (4 of the 4 ordered pairs appear).
All inputs are finite; a program needn't handle non-finite values.
Results may differ from the reference program's by a relative error of at most 0.00082.
Values may be sent and summed in bfloat16 or wider, within the bound.
A program may use at most 128 MiB of HBM per device.

```python
import jax
import jax.numpy as jnp
from jax import lax

NV = 192
NAUX = 768
KA_DEV = 2
ROUNDS = 2
NK = 32
NOCC = 2
NPAIRS = 4


def draw_conserve(key, part):
    groups = NK // KA_DEV
    row_keys = jax.random.split(jax.random.fold_in(key, 7), groups * ROUNDS)
    orders = jax.vmap(lambda single: jax.random.permutation(single, KA_DEV))(row_keys)
    orders = orders.reshape(groups, ROUNDS, KA_DEV).transpose(0, 2, 1).astype(jnp.int32)
    device = jnp.arange(groups, dtype=jnp.int32)[:, None, None]
    round_ids = jnp.arange(ROUNDS, dtype=jnp.int32)[None, None, :]
    source = (device - round_ids - 1) % groups
    mirror = source * KA_DEV + orders
    return ((NK - mirror) % NK).reshape(NK, ROUNDS).astype(jnp.int32)


def draw_pair_lists(key, part):
    square = NOCC * NOCC
    round_keys = jax.random.split(jax.random.fold_in(key, 11), ROUNDS)
    middle = jax.vmap(lambda single: jax.random.permutation(single, square - 2))(round_keys).astype(jnp.int32) + 1
    ends = jnp.broadcast_to(jnp.array([0, square - 1], dtype=jnp.int32)[None, :], (ROUNDS, 2))
    orders = jnp.concatenate([ends, middle], axis=1)
    positions = jnp.arange(NPAIRS, dtype=jnp.int32)
    picked = orders[:, positions % square]
    extra = jax.random.randint(jax.random.fold_in(key, 13), (ROUNDS, NPAIRS), 0, square).astype(jnp.int32)
    flat = jnp.where(positions[None, :] < square, picked, extra)
    leading = flat // NOCC
    trailing = flat % NOCC
    return jnp.stack([leading, trailing], axis=-1).astype(jnp.int32)


def block_levels(rng, dims, cuts, smallest, largest):
    def one(position, parts):
        steps = jax.random.uniform(jax.random.fold_in(jax.random.fold_in(rng, 6), position), (parts,), jnp.float32, smallest / len(cuts), largest / len(cuts))
        return jnp.repeat(jnp.exp(steps), dims[position] // parts).reshape((-1,) + (1,) * (len(dims) - position - 1))

    gain = one(*cuts[0])
    for cut in cuts[1:]:
        gain = gain * one(*cut)
    return gain


def normal_values(own_key, extent, spread, most, cuts=(), kind=jnp.bfloat16):
    entries = spread * jax.random.normal(own_key, extent, jnp.float32)
    if cuts:
        entries = entries * block_levels(own_key, extent, cuts, -0.22, 0.18)
    return jnp.clip(entries, -most, most).astype(kind)


def setup_inputs(seed: int = 0) -> dict:
    seeds = jax.random.split(jax.random.key(seed), 6)
    factors = normal_values(seeds[0], (NK, NOCC, NV, 2, NAUX), 0.04, 0.23925781, ((0, 16),))
    occupied_energy = jnp.clip(jax.random.uniform(seeds[1], (NOCC,), jnp.float32, -2.0, -0.5), -2.0, -0.5)
    virtual_energy = jnp.clip(0.5 + 2.5 * jax.random.uniform(seeds[2], (NK, NV), jnp.float32) ** block_levels(seeds[2], (NK, NV), ((0, 16),), -0.2, 0.2), 0.5, 3.0).astype(jnp.bfloat16)
    conserve = draw_conserve(jax.random.fold_in(seeds[5], 71), 0)
    pair_lists = draw_pair_lists(jax.random.fold_in(seeds[5], 71), 0)
    return {"factors": factors, "occupied_energy": occupied_energy, "virtual_energy": virtual_energy, "conserve": conserve, "pair_lists": pair_lists}


def build_mates(received, auxiliary):
    real_part = received[..., :auxiliary]
    imaginary = received[..., auxiliary:]
    turned = jnp.concatenate([-imaginary, real_part], axis=-1)
    return jnp.concatenate([received, turned], axis=-2)


def amplitude(left_rows, mate_rows, energy_left, energy_right, occupied_sum):
    values = lax.dot_general(left_rows, mate_rows, (((1,), (1,)), ((), ())), preferred_element_type=jnp.float32)
    denominator = energy_left[:, None] + energy_right[None, :] - occupied_sum
    return values / jnp.concatenate([denominator, denominator], axis=1)


def density_term(amplitudes, swapped):
    virtuals = amplitudes.shape[0]
    combined = (2.0 * amplitudes - swapped).astype(jnp.bfloat16)
    rounded = amplitudes.astype(jnp.bfloat16)
    turned = jnp.concatenate([-rounded[:, virtuals:], rounded[:, :virtuals]], axis=1)
    stacked = jnp.concatenate([rounded, turned], axis=0)
    return lax.dot_general(combined, stacked, (((1,), (1,)), ((), ())), preferred_element_type=jnp.float32)


def pair_term(own_block, mate_block, energy_left, energy_right, occupied_energy, pair_row):
    leading = pair_row[0]
    trailing = pair_row[1]
    occupied_sum = occupied_energy[leading] + occupied_energy[trailing]
    amplitudes = amplitude(own_block[leading], mate_block[trailing], energy_left, energy_right, occupied_sum)
    swapped = amplitude(own_block[trailing], mate_block[leading], energy_left, energy_right, occupied_sum)
    return density_term(amplitudes, swapped)


def reference(factors, occupied_energy, virtual_energy, conserve, pair_lists):
    momentum_count = factors.shape[0]
    orbitals = factors.shape[1]
    virtuals = factors.shape[2]
    auxiliary = factors.shape[4]
    stacked = factors.reshape(momentum_count, orbitals, virtuals, 2 * auxiliary)
    energies = virtual_energy.astype(jnp.float32)

    def one_momentum(moment):
        own_block = stacked[moment]
        energy_left = energies[moment]
        running = jnp.zeros((virtuals, 2 * virtuals), jnp.float32)
        for round_index in range(conserve.shape[1]):
            mirror = ((momentum_count - conserve[moment, round_index]) % momentum_count).astype(jnp.int32)
            mate_block = build_mates(stacked[mirror], auxiliary)
            energy_right = energies[mirror]

            def add_pair(partial_sum, pair_row):
                term = pair_term(own_block, mate_block, energy_left, energy_right, occupied_energy, pair_row)
                return partial_sum + term, None

            running, ignored = lax.scan(add_pair, running, pair_lists[round_index])
        return running.reshape(virtuals, 2, virtuals)

    return lax.map(one_momentum, jnp.arange(momentum_count, dtype=jnp.int32))
```

```python
import functools

import jax
import jax.numpy as jnp
from jax import lax
from jax.experimental import pallas as pl
from jax.experimental.pallas import tpu as pltpu
from jax.sharding import PartitionSpec as P

LANES = 128
BAND = 64
PIECE = 16


def from_behind(array, axis, by):
    size = lax.axis_size(axis)
    return lax.ppermute(array, axis, [(i, (i + by) % size) for i in range(size)])


def build_mates(received, auxiliary):
    real_part = received[..., :auxiliary]
    imaginary = received[..., auxiliary:]
    turned = jnp.concatenate([-imaginary, real_part], axis=-1)
    return jnp.concatenate([received, turned], axis=-2)


def amplitude(left_rows, mate_rows, energy_left, energy_right, occupied_sum):
    values = lax.dot_general(
        left_rows, mate_rows, (((1,), (1,)), ((), ())), preferred_element_type=jnp.float32
    )
    denominator = energy_left[:, None] + energy_right[None, :] - occupied_sum
    return values / jnp.concatenate([denominator, denominator], axis=1)


def density_term(amplitudes, swapped):
    virtuals = amplitudes.shape[0]
    combined = (2.0 * amplitudes - swapped).astype(jnp.bfloat16)
    rounded = amplitudes.astype(jnp.bfloat16)
    turned = jnp.concatenate([-rounded[:, virtuals:], rounded[:, :virtuals]], axis=1)
    stacked = jnp.concatenate([rounded, turned], axis=0)
    return lax.dot_general(
        combined, stacked, (((1,), (1,)), ((), ())), preferred_element_type=jnp.float32
    )


def pair_term(own_block, mate_block, energy_left, energy_right, occupied_energy, pair_row):
    leading = pair_row[0]
    trailing = pair_row[1]
    occupied_sum = occupied_energy[leading] + occupied_energy[trailing]
    amplitudes = amplitude(
        own_block[leading], mate_block[trailing], energy_left, energy_right, occupied_sum
    )
    swapped = amplitude(
        own_block[trailing], mate_block[leading], energy_left, energy_right, occupied_sum
    )
    return density_term(amplitudes, swapped)


def general(factors, occupied_energy, virtual_energy, conserve, pair_lists):
    momenta = factors.shape[0]
    orbitals = factors.shape[1]
    virtuals = factors.shape[2]
    auxiliary = factors.shape[4]
    own = factors.reshape(momenta, orbitals, virtuals, 2 * auxiliary)
    energy_own = virtual_energy.astype(jnp.float32)
    density = jnp.zeros((momenta, virtuals, 2 * virtuals), jnp.float32)
    for round_index in range(conserve.shape[1]):
        portion = orbitals // lax.axis_size("occ")
        portion_block = lax.dynamic_slice_in_dim(
            factors, lax.axis_index("occ") * portion, portion, 1
        )
        shifted, energy_mate = from_behind((portion_block, virtual_energy), "ka", round_index + 1)
        received = lax.all_gather(shifted, "occ", axis=1, tiled=True)
        mates = build_mates(received.reshape(momenta, orbitals, virtuals, 2 * auxiliary), auxiliary)
        energy_mate = energy_mate.astype(jnp.float32)
        for local_index in range(momenta):
            chosen = (momenta - conserve[local_index, round_index] % momenta) % momenta
            mate_block = lax.dynamic_index_in_dim(mates, chosen, 0, keepdims=False)
            energy_right = lax.dynamic_index_in_dim(energy_mate, chosen, 0, keepdims=False)
            own_block = own[local_index]
            energy_left = energy_own[local_index]

            def add_pair(partial_sum, pair_row):
                term = pair_term(
                    own_block, mate_block, energy_left, energy_right, occupied_energy, pair_row
                )
                return (partial_sum + term, None)

            running, ignored = lax.scan(add_pair, density[local_index], pair_lists[round_index])
            density = density.at[local_index].set(running)
    shaped = density.reshape(momenta, virtuals, 2, virtuals)
    return lax.psum_scatter(shaped, "occ", scatter_dimension=1, tiled=True)


def fused_kernel(
    ring, virtuals, strips,
    conserve_ref, occupied_ref, energy_ref, factors_ref, out_ref,
    own_raw, mate_raw, wide, own, mate, energy_in, energy_left, energy_rows, products, total, incoming,
    own_sem, far_send, far_recv, near_send, near_recv,
    energy_send, energy_recv, swap_send, swap_recv,
):
    mesh_id = pl.DeviceIdType.MESH
    me = lax.axis_index("ka")
    core = lax.axis_index("occ")
    other = 1 - core
    odd = lax.rem(me, 2)
    span = 2 * strips
    half = virtuals // 2
    pieces = virtuals // PIECE
    bands = virtuals // BAND
    subs = BAND // PIECE

    def at(step):
        return lax.rem(me + step + ring, ring)

    near = at(1 - 2 * odd)

    own_copy = pltpu.make_async_copy(factors_ref, own_raw, own_sem)
    own_copy.start()

    barrier = pltpu.get_barrier_semaphore()
    for step in (1, 2, -1, -2):
        pl.semaphore_signal(barrier, inc=1, device_id=(at(step), core), device_id_type=mesh_id)
    pl.semaphore_signal(barrier, inc=1, device_id=(me, other), device_id_type=mesh_id)
    pl.semaphore_wait(barrier, 5)

    def rows_of(piece):
        return pl.ds(pl.multiple_of(piece * (PIECE * span), PIECE * span), PIECE * span)

    def far_copy(piece):
        return pltpu.make_async_remote_copy(
            src_ref=factors_ref.at[core, :, rows_of(piece), :],
            dst_ref=mate_raw.at[1, :, rows_of(piece), :],
            send_sem=far_send.at[piece], recv_sem=far_recv.at[piece],
            device_id=(at(2), core), device_id_type=mesh_id,
        )

    def near_copy(piece, relay):
        source = mate_raw.at[1] if relay else factors_ref.at[core]
        return pltpu.make_async_remote_copy(
            src_ref=source.at[:, rows_of(piece), :],
            dst_ref=mate_raw.at[0, :, rows_of(piece), :],
            send_sem=near_send.at[piece], recv_sem=near_recv.at[piece],
            device_id=(near, core), device_id_type=mesh_id,
        )

    def energy_copy(slot):
        return pltpu.make_async_remote_copy(
            src_ref=energy_ref, dst_ref=energy_in.at[slot],
            send_sem=energy_send.at[slot], recv_sem=energy_recv.at[slot],
            device_id=(at(slot + 1), core), device_id_type=mesh_id,
        )

    energy_copy(0).start()
    energy_copy(1).start()

    def send_piece(piece, carry):
        far_copy(piece).start()

        @pl.when(odd == 0)
        def _():
            near_copy(piece, False).start()

        return carry

    lax.fori_loop(0, pieces, send_piece, 0)

    chosen = []
    for slot in range(2):
        mirror = lax.rem(2 - lax.rem(conserve_ref[0, slot], 2), 2)
        chosen.append(jnp.where(mirror == core, 0, 1))

    total[...] = jnp.zeros_like(total)
    own_copy.wait()

    def shape_own(step, carry):
        momentum_orbital = step // pieces
        piece = lax.rem(step, pieces)
        momentum = momentum_orbital // 2
        orbital = lax.rem(momentum_orbital, 2)
        wide[...] = own_raw[momentum, orbital, rows_of(piece), :].astype(jnp.float32)
        row = pl.ds(pl.multiple_of(orbital * virtuals + piece * PIECE, PIECE), PIECE)
        for column in range(span):
            block = wide[pl.ds(column, PIECE, stride=span), :].astype(jnp.bfloat16)
            own[momentum, row, pl.ds(column * LANES, LANES)] = block
        return carry

    lax.fori_loop(0, 4 * pieces, shape_own, 0)

    diagonal = lax.broadcasted_iota(jnp.int32, (virtuals, virtuals), 0) == lax.broadcasted_iota(
        jnp.int32, (virtuals, virtuals), 1
    )
    mine = energy_ref[...].astype(jnp.float32)
    for momentum in range(2):
        spread = jnp.where(diagonal, mine[momentum : momentum + 1, :], 0.0)
        column = jnp.sum(spread, axis=1, keepdims=True)
        energy_left[momentum] = jnp.broadcast_to(column, (virtuals, LANES))
    for slot in range(2):
        energy_copy(slot).wait()
        theirs = energy_in[slot].astype(jnp.float32)
        theirs = jnp.where(core == 0, theirs[0:1, :], theirs[1:2, :])
        for band in range(bands):
            part = theirs[:, band * BAND : (band + 1) * BAND]
            energy_rows[slot, band] = jnp.broadcast_to(
                jnp.concatenate([part, part], axis=1), (8, LANES)
            )

    sign = jnp.where(lax.broadcasted_iota(jnp.int32, (virtuals, LANES), 1) < BAND, -1.0, 1.0)

    def shape_mate(slot, piece, sub):
        for orbital in range(2):
            wide[...] = mate_raw[slot, orbital, rows_of(piece), :].astype(jnp.float32)
            first = orbital * 2 * BAND + sub * PIECE
            plain = pl.ds(pl.multiple_of(first, PIECE), PIECE)
            turned = pl.ds(pl.multiple_of(first + BAND, PIECE), PIECE)
            for strip in range(strips):
                real = wide[pl.ds(2 * strip, PIECE, stride=span), :]
                imaginary = wide[pl.ds(2 * strip + 1, PIECE, stride=span), :]
                left = pl.ds(2 * strip * LANES, LANES)
                right = pl.ds((2 * strip + 1) * LANES, LANES)
                mate[slot, plain, left] = real.astype(jnp.bfloat16)
                mate[slot, plain, right] = imaginary.astype(jnp.bfloat16)
                mate[slot, turned, left] = (-imaginary).astype(jnp.bfloat16)
                mate[slot, turned, right] = real.astype(jnp.bfloat16)

    def add_band(slot, band):
        momentum = chosen[slot]
        products[...] = lax.dot_general(
            own[momentum], mate[slot], (((1,), (1,)), ((), ())), preferred_element_type=jnp.float32
        )
        base = energy_left[momentum] + energy_rows[slot, band][0:1, :]
        amplitudes = {}
        for i in range(2):
            for j in range(2):
                gap = base - (occupied_ref[i] + occupied_ref[j])
                value = products[i * virtuals : (i + 1) * virtuals, j * LANES : (j + 1) * LANES]
                amplitudes[i, j] = value / gap
        combined, rounded, turned = [], [], []
        for i in range(2):
            for j in range(2):
                this = amplitudes[i, j]
                combined.append((2.0 * this - amplitudes[j, i]).astype(jnp.bfloat16))
                rounded.append(this.astype(jnp.bfloat16))
                turned.append((pltpu.roll(this, BAND, 1) * sign).astype(jnp.bfloat16))
        left = jnp.concatenate(combined, axis=1)
        right = jnp.concatenate(
            [jnp.concatenate(rounded, axis=1), jnp.concatenate(turned, axis=1)], axis=0
        )
        total[slot] += lax.dot_general(
            left, right, (((1,), (1,)), ((), ())), preferred_element_type=jnp.float32
        )

    def band_step(band, carry):
        def piece_step(sub, inner):
            piece = band * subs + sub
            far_copy(piece).wait_recv()

            @pl.when(odd == 1)
            def _():
                near_copy(piece, True).start()

            shape_mate(1, piece, sub)
            near_copy(piece, False).wait_recv()
            shape_mate(0, piece, sub)
            return inner

        lax.fori_loop(0, subs, piece_step, 0)
        add_band(1, band)
        add_band(0, band)
        return carry

    lax.fori_loop(0, bands, band_step, 0)

    def swap_copy(slot):
        return pltpu.make_async_remote_copy(
            src_ref=total.at[slot, pl.ds(pl.multiple_of(other * half, half), half), :],
            dst_ref=incoming.at[slot],
            send_sem=swap_send.at[slot], recv_sem=swap_recv.at[slot],
            device_id=(me, other), device_id_type=mesh_id,
        )

    for slot in (1, 0):
        swap_copy(slot).start()
    for slot in (1, 0):
        swap_copy(slot).wait()

    here = pl.ds(pl.multiple_of(core * half, half), half)
    for momentum in range(2):
        value = jnp.zeros((half, 2 * virtuals), jnp.float32)
        for slot in (1, 0):
            value += jnp.where(chosen[slot] == momentum, total[slot, here, :], incoming[slot])
        for part in range(2):
            out_ref[momentum, :, part, :] = value[:, part * virtuals : (part + 1) * virtuals]

    def drain(piece, carry):
        far_copy(piece).wait_send()
        near_copy(piece, False).wait_send()
        return carry

    lax.fori_loop(0, pieces, drain, 0)


def fused(factors, occupied_energy, virtual_energy, conserve, pair_lists):
    momenta, orbitals, virtuals, parts, auxiliary = factors.shape
    strips = auxiliary // LANES
    ring = lax.axis_size("ka")
    raw_rows = virtuals * parts * strips
    raw = factors.reshape(momenta, orbitals, virtuals, parts, strips, LANES)
    raw = raw.transpose(0, 1, 2, 4, 3, 5).reshape(momenta, orbitals, raw_rows, LANES)
    pieces = virtuals // PIECE
    dma = pltpu.SemaphoreType.DMA
    return pl.pallas_call(
        functools.partial(fused_kernel, ring, virtuals, strips),
        out_shape=jax.ShapeDtypeStruct((momenta, virtuals // 2, 2, virtuals), jnp.float32),
        in_specs=[
            pl.BlockSpec(memory_space=pltpu.SMEM),
            pl.BlockSpec(memory_space=pltpu.SMEM),
            pl.BlockSpec(memory_space=pltpu.VMEM),
            pl.BlockSpec(memory_space=pl.ANY),
        ],
        out_specs=pl.BlockSpec(memory_space=pltpu.VMEM),
        scratch_shapes=[
            pltpu.VMEM((momenta, orbitals, raw_rows, LANES), jnp.bfloat16),
            pltpu.VMEM((2, orbitals, raw_rows, LANES), jnp.bfloat16),
            pltpu.VMEM((PIECE * parts * strips, LANES), jnp.float32),
            pltpu.VMEM((momenta, orbitals * virtuals, parts * auxiliary), jnp.bfloat16),
            pltpu.VMEM((2, orbitals * 2 * BAND, parts * auxiliary), jnp.bfloat16),
            pltpu.VMEM((2, momenta, virtuals), jnp.bfloat16),
            pltpu.VMEM((momenta, virtuals, LANES), jnp.float32),
            pltpu.VMEM((2, virtuals // BAND, 8, LANES), jnp.float32),
            pltpu.VMEM((orbitals * virtuals, orbitals * 2 * BAND), jnp.float32),
            pltpu.VMEM((2, virtuals, 2 * virtuals), jnp.float32),
            pltpu.VMEM((2, virtuals // 2, 2 * virtuals), jnp.float32),
            dma,
            dma((pieces,)), dma((pieces,)), dma((pieces,)), dma((pieces,)),
            dma((2,)), dma((2,)), dma((2,)), dma((2,)),
        ],
        compiler_params=pltpu.CompilerParams(
            collective_id=0, has_side_effects=True, vmem_limit_bytes=48 * 1024 * 1024
        ),
        name="density",
    )(conserve, occupied_energy, virtual_energy, raw)


def local(factors, occupied_energy, virtual_energy, conserve, pair_lists):
    momenta, orbitals, virtuals, parts, auxiliary = factors.shape
    rounds, pairs = pair_lists.shape[:2]
    ring, holders = lax.axis_size("ka"), lax.axis_size("occ")
    whole_square = pairs * holders == orbitals * orbitals
    fits = momenta == 2 and orbitals == 2 and holders == 2 and rounds == 2
    even = ring % 2 == 0 and ring > 4 and virtuals % BAND == 0 and auxiliary % LANES == 0
    chosen = fused if whole_square and fits and even else general
    return chosen(factors, occupied_energy, virtual_energy, conserve, pair_lists)


def solution(mesh):
    in_specs = (
        P("ka", None, None, None, None),
        P(),
        P("ka", None),
        P("ka", None),
        P(None, "occ", None),
    )
    out_specs = P("ka", "occ", None, None)
    return jax.shard_map(local, mesh=mesh, in_specs=in_specs, out_specs=out_specs, check_vma=False)
```

```python
import functools

import jax
import jax.numpy as jnp
from jax import lax
from jax.experimental import pallas as pl
from jax.experimental.pallas import tpu as pltpu
from jax.sharding import PartitionSpec as P

LANES = 128
BAND = 64
STEP = 16
PIECE = 8


def from_behind(array, axis, by):
    size = lax.axis_size(axis)
    return lax.ppermute(array, axis, [(i, (i + by) % size) for i in range(size)])


def build_mates(received, auxiliary):
    real_part = received[..., :auxiliary]
    imaginary = received[..., auxiliary:]
    turned = jnp.concatenate([-imaginary, real_part], axis=-1)
    return jnp.concatenate([received, turned], axis=-2)


def amplitude(left_rows, mate_rows, energy_left, energy_right, occupied_sum):
    values = lax.dot_general(
        left_rows, mate_rows, (((1,), (1,)), ((), ())), preferred_element_type=jnp.float32
    )
    denominator = energy_left[:, None] + energy_right[None, :] - occupied_sum
    return values / jnp.concatenate([denominator, denominator], axis=1)


def density_term(amplitudes, swapped):
    virtuals = amplitudes.shape[0]
    combined = (2.0 * amplitudes - swapped).astype(jnp.bfloat16)
    rounded = amplitudes.astype(jnp.bfloat16)
    turned = jnp.concatenate([-rounded[:, virtuals:], rounded[:, :virtuals]], axis=1)
    stacked = jnp.concatenate([rounded, turned], axis=0)
    return lax.dot_general(
        combined, stacked, (((1,), (1,)), ((), ())), preferred_element_type=jnp.float32
    )


def pair_term(own_block, mate_block, energy_left, energy_right, occupied_energy, pair_row):
    leading = pair_row[0]
    trailing = pair_row[1]
    occupied_sum = occupied_energy[leading] + occupied_energy[trailing]
    amplitudes = amplitude(
        own_block[leading], mate_block[trailing], energy_left, energy_right, occupied_sum
    )
    swapped = amplitude(
        own_block[trailing], mate_block[leading], energy_left, energy_right, occupied_sum
    )
    return density_term(amplitudes, swapped)


def general(factors, occupied_energy, virtual_energy, conserve, pair_lists):
    momenta = factors.shape[0]
    orbitals = factors.shape[1]
    virtuals = factors.shape[2]
    auxiliary = factors.shape[4]
    own = factors.reshape(momenta, orbitals, virtuals, 2 * auxiliary)
    energy_own = virtual_energy.astype(jnp.float32)
    density = jnp.zeros((momenta, virtuals, 2 * virtuals), jnp.float32)
    for round_index in range(conserve.shape[1]):
        portion = orbitals // lax.axis_size("occ")
        portion_block = lax.dynamic_slice_in_dim(
            factors, lax.axis_index("occ") * portion, portion, 1
        )
        shifted, energy_mate = from_behind((portion_block, virtual_energy), "ka", round_index + 1)
        received = lax.all_gather(shifted, "occ", axis=1, tiled=True)
        mates = build_mates(received.reshape(momenta, orbitals, virtuals, 2 * auxiliary), auxiliary)
        energy_mate = energy_mate.astype(jnp.float32)
        for local_index in range(momenta):
            chosen = (momenta - conserve[local_index, round_index] % momenta) % momenta
            mate_block = lax.dynamic_index_in_dim(mates, chosen, 0, keepdims=False)
            energy_right = lax.dynamic_index_in_dim(energy_mate, chosen, 0, keepdims=False)
            own_block = own[local_index]
            energy_left = energy_own[local_index]

            def add_pair(partial_sum, pair_row):
                term = pair_term(
                    own_block, mate_block, energy_left, energy_right, occupied_energy, pair_row
                )
                return (partial_sum + term, None)

            running, ignored = lax.scan(add_pair, density[local_index], pair_lists[round_index])
            density = density.at[local_index].set(running)
    shaped = density.reshape(momenta, virtuals, 2, virtuals)
    return lax.psum_scatter(shaped, "occ", scatter_dimension=1, tiled=True)


def fused_kernel(
    ring, virtuals, auxiliary,
    conserve_ref, occupied_ref, energy_ref, factors_ref, out_ref,
    own_raw, mate_raw, own, mate, energy_in, energy_left, energy_rows, products, total, incoming,
    own_sem, far_send, far_recv, near_send, near_recv,
    energy_send, energy_recv, swap_send, swap_recv,
):
    mesh_id = pl.DeviceIdType.MESH
    me = lax.axis_index("ka")
    core = lax.axis_index("occ")
    other = 1 - core
    odd = lax.rem(me, 2)
    half = virtuals // 2
    pieces = virtuals // PIECE
    steps = virtuals // STEP
    bands = virtuals // BAND
    per_step = STEP // PIECE
    per_band = BAND // STEP

    def at(step):
        return lax.rem(me + step + ring, ring)

    near = at(1 - 2 * odd)

    def own_copy(momentum, index):
        return pltpu.make_async_copy(
            factors_ref.at[momentum], own_raw.at[momentum], own_sem.at[index]
        )

    own_copy(core, 0).start()
    own_copy(other, 1).start()

    barrier = pltpu.get_barrier_semaphore()
    for step in (1, 2, -1, -2):
        pl.semaphore_signal(barrier, inc=1, device_id=(at(step), core), device_id_type=mesh_id)
    pl.semaphore_signal(barrier, inc=1, device_id=(me, other), device_id_type=mesh_id)

    def piece_rows(piece):
        return pl.ds(pl.multiple_of(piece * PIECE, PIECE), PIECE)

    def step_rows(step):
        return pl.ds(pl.multiple_of(step * STEP, STEP), STEP)

    def far_copy(piece):
        return pltpu.make_async_remote_copy(
            src_ref=own_raw.at[core, :, piece_rows(piece)],
            dst_ref=mate_raw.at[1, :, piece_rows(piece)],
            send_sem=far_send.at[piece], recv_sem=far_recv.at[piece],
            device_id=(at(2), core), device_id_type=mesh_id,
        )

    def near_copy(piece, relay):
        source = mate_raw.at[1] if relay else own_raw.at[core]
        return pltpu.make_async_remote_copy(
            src_ref=source.at[:, piece_rows(piece)],
            dst_ref=mate_raw.at[0, :, piece_rows(piece)],
            send_sem=near_send.at[piece], recv_sem=near_recv.at[piece],
            device_id=(near, core), device_id_type=mesh_id,
        )

    def energy_copy(slot):
        return pltpu.make_async_remote_copy(
            src_ref=energy_ref, dst_ref=energy_in.at[slot],
            send_sem=energy_send.at[slot], recv_sem=energy_recv.at[slot],
            device_id=(at(slot + 1), core), device_id_type=mesh_id,
        )

    own_copy(core, 0).wait()
    pl.semaphore_wait(barrier, 5)

    def send_piece(piece, carry):
        far_copy(piece).start()

        @pl.when(odd == 0)
        def _():
            near_copy(piece, False).start()

        return carry

    lax.fori_loop(0, 2, send_piece, 0)
    energy_copy(0).start()
    energy_copy(1).start()
    lax.fori_loop(2, pieces, send_piece, 0)

    chosen = []
    for slot in range(2):
        mirror = lax.rem(2 - lax.rem(conserve_ref[0, slot], 2), 2)
        chosen.append(jnp.where(mirror == core, 0, 1))

    own_copy(other, 1).wait()

    def forward(piece):
        far_copy(piece).wait_recv()

        @pl.when(odd == 1)
        def _():
            near_copy(piece, True).start()

    def shape_own(step, carry):
        for momentum in range(2):
            for orbital in range(2):
                row = pl.ds(pl.multiple_of(orbital * virtuals + step * STEP, STEP), STEP)
                for part in range(2):
                    own[momentum, row, pl.ds(part * auxiliary, auxiliary)] = own_raw[
                        momentum, orbital, step_rows(step), part, :
                    ]
        return carry

    def shape_mate(slot, step):
        band = step // per_band
        for orbital in range(2):
            real = mate_raw[slot, orbital, step_rows(step), 0, :]
            imaginary = mate_raw[slot, orbital, step_rows(step), 1, :]
            first = orbital * 2 * BAND + lax.rem(step, per_band) * STEP
            plain = pl.ds(pl.multiple_of(first, STEP), STEP)
            turned = pl.ds(pl.multiple_of(first + BAND, STEP), STEP)
            mate[slot, band, plain, pl.ds(0, auxiliary)] = real
            mate[slot, band, plain, pl.ds(auxiliary, auxiliary)] = imaginary
            mate[slot, band, turned, pl.ds(0, auxiliary)] = -imaginary
            mate[slot, band, turned, pl.ds(auxiliary, auxiliary)] = real

    def shape_energies():
        diagonal = lax.broadcasted_iota(
            jnp.int32, (virtuals, virtuals), 0
        ) == lax.broadcasted_iota(jnp.int32, (virtuals, virtuals), 1)
        mine = energy_ref[...].astype(jnp.float32)
        for momentum in range(2):
            spread = jnp.where(diagonal, mine[momentum : momentum + 1, :], 0.0)
            column = jnp.sum(spread, axis=1, keepdims=True)
            energy_left[momentum] = jnp.broadcast_to(column, (virtuals, LANES))
        for slot in range(2):
            energy_copy(slot).wait()
            theirs = energy_in[slot].astype(jnp.float32)
            theirs = jnp.where(core == 0, theirs[0:1, :], theirs[1:2, :])
            for band in range(bands):
                part = theirs[:, band * BAND : (band + 1) * BAND]
                energy_rows[slot, band] = jnp.broadcast_to(
                    jnp.concatenate([part, part], axis=1), (8, LANES)
                )

    sign = jnp.where(lax.broadcasted_iota(jnp.int32, (virtuals, LANES), 1) < BAND, -1.0, 1.0)

    def add_band(slot, band):
        momentum = jnp.where(slot == 1, chosen[1], chosen[0])
        products[...] = lax.dot_general(
            own[momentum], mate[slot, band], (((1,), (1,)), ((), ())),
            preferred_element_type=jnp.float32,
        )
        base = energy_left[momentum] + energy_rows[slot, band][0:1, :]
        amplitudes = {}
        for i in range(2):
            for j in range(2):
                gap = base - (occupied_ref[i] + occupied_ref[j])
                value = products[i * virtuals : (i + 1) * virtuals, j * LANES : (j + 1) * LANES]
                amplitudes[i, j] = value / gap
        combined, rounded, turned = [], [], []
        for i in range(2):
            for j in range(2):
                this = amplitudes[i, j]
                combined.append((2.0 * this - amplitudes[j, i]).astype(jnp.bfloat16))
                rounded.append(this.astype(jnp.bfloat16))
                turned.append((pltpu.roll(this, BAND, 1) * sign).astype(jnp.bfloat16))
        left = jnp.concatenate(combined, axis=1)
        right = jnp.concatenate(
            [jnp.concatenate(rounded, axis=1), jnp.concatenate(turned, axis=1)], axis=0
        )
        total[slot] += lax.dot_general(
            left, right, (((1,), (1,)), ((), ())), preferred_element_type=jnp.float32
        )

    def far_step(step):
        for piece in range(per_step):
            forward(step * per_step + piece)
        shape_mate(1, step)

    def near_step(step):
        for piece in range(per_step):
            near_copy(step * per_step + piece, False).wait_recv()
        shape_mate(0, step)

    total[...] = jnp.zeros_like(total)
    lax.fori_loop(0, steps // 2, shape_own, 0)
    far_step(0)
    lax.fori_loop(steps // 2, steps, shape_own, 0)
    shape_energies()

    def main_step(step, carry):
        far_step(step)
        near_step(step - 1)
        phase = lax.rem(step, per_band)
        ready = jnp.logical_and(step >= per_band, jnp.logical_or(phase == 1, phase == 2))

        @pl.when(ready)
        def _():
            add_band(2 - phase, step // per_band - 1)

        return carry

    lax.fori_loop(1, steps, main_step, 0)

    def swap_copy(slot):
        return pltpu.make_async_remote_copy(
            src_ref=total.at[slot, pl.ds(pl.multiple_of(other * half, half), half), :],
            dst_ref=incoming.at[slot],
            send_sem=swap_send.at[slot], recv_sem=swap_recv.at[slot],
            device_id=(me, other), device_id_type=mesh_id,
        )

    add_band(1, bands - 1)
    swap_copy(1).start()
    near_step(steps - 1)
    add_band(0, bands - 1)
    swap_copy(0).start()

    def drain(piece, carry):
        far_copy(piece).wait_send()
        near_copy(piece, False).wait_send()
        return carry

    lax.fori_loop(0, pieces, drain, 0)
    for slot in (1, 0):
        swap_copy(slot).wait()

    here = pl.ds(pl.multiple_of(core * half, half), half)
    for momentum in range(2):
        value = jnp.zeros((half, 2 * virtuals), jnp.float32)
        for slot in (1, 0):
            value += jnp.where(chosen[slot] == momentum, total[slot, here, :], incoming[slot])
        for part in range(2):
            out_ref[momentum, :, part, :] = value[:, part * virtuals : (part + 1) * virtuals]


def fused(factors, occupied_energy, virtual_energy, conserve, pair_lists):
    momenta, orbitals, virtuals, parts, auxiliary = factors.shape
    ring = lax.axis_size("ka")
    pieces = virtuals // PIECE
    bands = virtuals // BAND
    dma = pltpu.SemaphoreType.DMA
    return pl.pallas_call(
        functools.partial(fused_kernel, ring, virtuals, auxiliary),
        out_shape=jax.ShapeDtypeStruct((momenta, virtuals // 2, 2, virtuals), jnp.float32),
        in_specs=[
            pl.BlockSpec(memory_space=pltpu.SMEM),
            pl.BlockSpec(memory_space=pltpu.SMEM),
            pl.BlockSpec(memory_space=pltpu.VMEM),
            pl.BlockSpec(memory_space=pl.ANY),
        ],
        out_specs=pl.BlockSpec(memory_space=pltpu.VMEM),
        scratch_shapes=[
            pltpu.VMEM((momenta, orbitals, virtuals, parts, auxiliary), jnp.bfloat16),
            pltpu.VMEM((2, orbitals, virtuals, parts, auxiliary), jnp.bfloat16),
            pltpu.VMEM((momenta, orbitals * virtuals, parts * auxiliary), jnp.bfloat16),
            pltpu.VMEM((2, bands, orbitals * 2 * BAND, parts * auxiliary), jnp.bfloat16),
            pltpu.VMEM((2, momenta, virtuals), jnp.bfloat16),
            pltpu.VMEM((momenta, virtuals, LANES), jnp.float32),
            pltpu.VMEM((2, bands, 8, LANES), jnp.float32),
            pltpu.VMEM((orbitals * virtuals, orbitals * 2 * BAND), jnp.float32),
            pltpu.VMEM((2, virtuals, 2 * virtuals), jnp.float32),
            pltpu.VMEM((2, virtuals // 2, 2 * virtuals), jnp.float32),
            dma((2,)),
            dma((pieces,)), dma((pieces,)), dma((pieces,)), dma((pieces,)),
            dma((2,)), dma((2,)), dma((2,)), dma((2,)),
        ],
        compiler_params=pltpu.CompilerParams(
            collective_id=0, has_side_effects=True, vmem_limit_bytes=56 * 1024 * 1024
        ),
        name="density",
    )(conserve, occupied_energy, virtual_energy, factors)


def local(factors, occupied_energy, virtual_energy, conserve, pair_lists):
    momenta, orbitals, virtuals, parts, auxiliary = factors.shape
    rounds, pairs = pair_lists.shape[:2]
    ring, holders = lax.axis_size("ka"), lax.axis_size("occ")
    whole_square = pairs * holders == orbitals * orbitals
    fits = momenta == 2 and orbitals == 2 and holders == 2 and rounds == 2
    even = ring % 2 == 0 and ring > 4 and virtuals % BAND == 0 and auxiliary % LANES == 0
    chosen = fused if whole_square and fits and even else general
    return chosen(factors, occupied_energy, virtual_energy, conserve, pair_lists)


def solution(mesh):
    in_specs = (
        P("ka", None, None, None, None),
        P(),
        P("ka", None),
        P("ka", None),
        P(None, "occ", None),
    )
    out_specs = P("ka", "occ", None, None)
    return jax.shard_map(local, mesh=mesh, in_specs=in_specs, out_specs=out_specs, check_vma=False)
```

```python
import functools

import jax
import jax.numpy as jnp
from jax import lax
from jax.experimental import pallas as pl
from jax.experimental.pallas import tpu as pltpu
from jax.sharding import PartitionSpec as P

LANES = 128
BAND = 64
STEP = 16
PIECE = 8


def from_behind(array, axis, by):
    size = lax.axis_size(axis)
    return lax.ppermute(array, axis, [(i, (i + by) % size) for i in range(size)])


def build_mates(received, auxiliary):
    real_part = received[..., :auxiliary]
    imaginary = received[..., auxiliary:]
    turned = jnp.concatenate([-imaginary, real_part], axis=-1)
    return jnp.concatenate([received, turned], axis=-2)


def amplitude(left_rows, mate_rows, energy_left, energy_right, occupied_sum):
    values = lax.dot_general(
        left_rows, mate_rows, (((1,), (1,)), ((), ())), preferred_element_type=jnp.float32
    )
    denominator = energy_left[:, None] + energy_right[None, :] - occupied_sum
    return values / jnp.concatenate([denominator, denominator], axis=1)


def density_term(amplitudes, swapped):
    virtuals = amplitudes.shape[0]
    combined = (2.0 * amplitudes - swapped).astype(jnp.bfloat16)
    rounded = amplitudes.astype(jnp.bfloat16)
    turned = jnp.concatenate([-rounded[:, virtuals:], rounded[:, :virtuals]], axis=1)
    stacked = jnp.concatenate([rounded, turned], axis=0)
    return lax.dot_general(
        combined, stacked, (((1,), (1,)), ((), ())), preferred_element_type=jnp.float32
    )


def pair_term(own_block, mate_block, energy_left, energy_right, occupied_energy, pair_row):
    leading = pair_row[0]
    trailing = pair_row[1]
    occupied_sum = occupied_energy[leading] + occupied_energy[trailing]
    amplitudes = amplitude(
        own_block[leading], mate_block[trailing], energy_left, energy_right, occupied_sum
    )
    swapped = amplitude(
        own_block[trailing], mate_block[leading], energy_left, energy_right, occupied_sum
    )
    return density_term(amplitudes, swapped)


def general(factors, occupied_energy, virtual_energy, conserve, pair_lists):
    momenta = factors.shape[0]
    orbitals = factors.shape[1]
    virtuals = factors.shape[2]
    auxiliary = factors.shape[4]
    own = factors.reshape(momenta, orbitals, virtuals, 2 * auxiliary)
    energy_own = virtual_energy.astype(jnp.float32)
    density = jnp.zeros((momenta, virtuals, 2 * virtuals), jnp.float32)
    for round_index in range(conserve.shape[1]):
        portion = orbitals // lax.axis_size("occ")
        portion_block = lax.dynamic_slice_in_dim(
            factors, lax.axis_index("occ") * portion, portion, 1
        )
        shifted, energy_mate = from_behind((portion_block, virtual_energy), "ka", round_index + 1)
        received = lax.all_gather(shifted, "occ", axis=1, tiled=True)
        mates = build_mates(received.reshape(momenta, orbitals, virtuals, 2 * auxiliary), auxiliary)
        energy_mate = energy_mate.astype(jnp.float32)
        for local_index in range(momenta):
            chosen = (momenta - conserve[local_index, round_index] % momenta) % momenta
            mate_block = lax.dynamic_index_in_dim(mates, chosen, 0, keepdims=False)
            energy_right = lax.dynamic_index_in_dim(energy_mate, chosen, 0, keepdims=False)
            own_block = own[local_index]
            energy_left = energy_own[local_index]

            def add_pair(partial_sum, pair_row):
                term = pair_term(
                    own_block, mate_block, energy_left, energy_right, occupied_energy, pair_row
                )
                return (partial_sum + term, None)

            running, ignored = lax.scan(add_pair, density[local_index], pair_lists[round_index])
            density = density.at[local_index].set(running)
    shaped = density.reshape(momenta, virtuals, 2, virtuals)
    return lax.psum_scatter(shaped, "occ", scatter_dimension=1, tiled=True)


def fused_kernel(
    ring, virtuals, auxiliary,
    conserve_hbm, occupied_hbm, energy_hbm, factors_ref, out_ref,
    conserve_ref, occupied_ref, energy_ref, own_raw, mate_raw, own, mate, energy_in, energy_left, energy_rows, products, total, incoming,
    small_sem, own_sem, far_send, far_recv, near_send, near_recv,
    energy_send, energy_recv, swap_send, swap_recv,
):
    mesh_id = pl.DeviceIdType.MESH
    me = lax.axis_index("ka")
    core = lax.axis_index("occ")
    other = 1 - core
    odd = lax.rem(me, 2)
    half = virtuals // 2
    pieces = virtuals // PIECE
    steps = virtuals // STEP
    bands = virtuals // BAND
    per_step = STEP // PIECE
    per_band = BAND // STEP

    def at(step):
        return lax.rem(me + step + ring, ring)

    near = at(1 - 2 * odd)

    def own_copy(momentum, index):
        return pltpu.make_async_copy(
            factors_ref.at[momentum], own_raw.at[momentum], own_sem.at[index]
        )

    def small_copies():
        return (
            pltpu.make_async_copy(conserve_hbm, conserve_ref, small_sem.at[0]),
            pltpu.make_async_copy(occupied_hbm, occupied_ref, small_sem.at[1]),
            pltpu.make_async_copy(energy_hbm, energy_ref, small_sem.at[2]),
        )

    barrier = pltpu.get_barrier_semaphore()
    for place in ((at(-2), core), (near, core), (me, other)):
        pl.semaphore_signal(barrier, inc=1, device_id=place, device_id_type=mesh_id)
    own_copy(core, 0).start()
    for copy in small_copies():
        copy.start()
    own_copy(other, 1).start()

    def piece_rows(piece):
        return pl.ds(pl.multiple_of(piece * PIECE, PIECE), PIECE)

    def step_rows(step):
        return pl.ds(pl.multiple_of(step * STEP, STEP), STEP)

    def far_copy(piece):
        return pltpu.make_async_remote_copy(
            src_ref=own_raw.at[core, :, piece_rows(piece)],
            dst_ref=mate_raw.at[1, :, piece_rows(piece)],
            send_sem=far_send.at[piece], recv_sem=far_recv.at[piece],
            device_id=(at(2), core), device_id_type=mesh_id,
        )

    def near_copy(piece, relay):
        source = mate_raw.at[1] if relay else own_raw.at[core]
        return pltpu.make_async_remote_copy(
            src_ref=source.at[:, piece_rows(piece)],
            dst_ref=mate_raw.at[0, :, piece_rows(piece)],
            send_sem=near_send.at[piece], recv_sem=near_recv.at[piece],
            device_id=(near, core), device_id_type=mesh_id,
        )

    def energy_far():
        return pltpu.make_async_remote_copy(
            src_ref=energy_ref, dst_ref=energy_in.at[1],
            send_sem=energy_send.at[1], recv_sem=energy_recv.at[1],
            device_id=(at(2), core), device_id_type=mesh_id,
        )

    def energy_near(relay):
        return pltpu.make_async_remote_copy(
            src_ref=energy_in.at[1] if relay else energy_ref, dst_ref=energy_in.at[0],
            send_sem=energy_send.at[0], recv_sem=energy_recv.at[0],
            device_id=(near, core), device_id_type=mesh_id,
        )

    own_copy(core, 0).wait()
    pl.semaphore_wait(barrier, 3)

    def send_piece(piece, carry):
        far_copy(piece).start()

        @pl.when(odd == 0)
        def _():
            near_copy(piece, False).start()

        return carry

    lax.fori_loop(0, 2, send_piece, 0)
    for copy in small_copies():
        copy.wait()
    energy_far().start()

    @pl.when(odd == 0)
    def _():
        energy_near(False).start()

    lax.fori_loop(2, pieces, send_piece, 0)

    chosen = []
    for slot in range(2):
        mirror = lax.rem(2 - lax.rem(conserve_ref[0, slot], 2), 2)
        chosen.append(jnp.where(mirror == core, 0, 1))

    own_copy(other, 1).wait()

    def forward(piece):
        far_copy(piece).wait_recv()

        @pl.when(odd == 1)
        def _():
            near_copy(piece, True).start()

    def shape_own(step, carry):
        for momentum in range(2):
            for orbital in range(2):
                row = pl.ds(pl.multiple_of(orbital * virtuals + step * STEP, STEP), STEP)
                for part in range(2):
                    own[momentum, row, pl.ds(part * auxiliary, auxiliary)] = own_raw[
                        momentum, orbital, step_rows(step), part, :
                    ]
        return carry

    def shape_mate(slot, step):
        band = step // per_band
        for orbital in range(2):
            real = mate_raw[slot, orbital, step_rows(step), 0, :]
            imaginary = mate_raw[slot, orbital, step_rows(step), 1, :]
            first = orbital * 2 * BAND + lax.rem(step, per_band) * STEP
            plain = pl.ds(pl.multiple_of(first, STEP), STEP)
            turned = pl.ds(pl.multiple_of(first + BAND, STEP), STEP)
            mate[slot, band, plain, pl.ds(0, auxiliary)] = real
            mate[slot, band, plain, pl.ds(auxiliary, auxiliary)] = imaginary
            mate[slot, band, turned, pl.ds(0, auxiliary)] = -imaginary
            mate[slot, band, turned, pl.ds(auxiliary, auxiliary)] = real

    def shape_energies():
        diagonal = lax.broadcasted_iota(
            jnp.int32, (virtuals, virtuals), 0
        ) == lax.broadcasted_iota(jnp.int32, (virtuals, virtuals), 1)
        mine = energy_ref[...].astype(jnp.float32)
        for momentum in range(2):
            spread = jnp.where(diagonal, mine[momentum : momentum + 1, :], 0.0)
            column = jnp.sum(spread, axis=1, keepdims=True)
            energy_left[momentum] = jnp.broadcast_to(column, (virtuals, LANES))
        energy_near(False).wait_recv()
        for slot in range(2):
            theirs = energy_in[slot].astype(jnp.float32)
            theirs = jnp.where(core == 0, theirs[0:1, :], theirs[1:2, :])
            for band in range(bands):
                part = theirs[:, band * BAND : (band + 1) * BAND]
                energy_rows[slot, band] = jnp.broadcast_to(
                    jnp.concatenate([part, part], axis=1), (8, LANES)
                )

    sign = jnp.where(lax.broadcasted_iota(jnp.int32, (virtuals, LANES), 1) < BAND, -1.0, 1.0)

    def add_band(slot, band):
        momentum = jnp.where(slot == 1, chosen[1], chosen[0])
        products[...] = lax.dot_general(
            own[momentum], mate[slot, band], (((1,), (1,)), ((), ())),
            preferred_element_type=jnp.float32,
        )
        base = energy_left[momentum] + energy_rows[slot, band][0:1, :]
        amplitudes = {}
        for i in range(2):
            for j in range(2):
                gap = base - (occupied_ref[i] + occupied_ref[j])
                value = products[i * virtuals : (i + 1) * virtuals, j * LANES : (j + 1) * LANES]
                amplitudes[i, j] = value / gap
        combined, rounded, turned = [], [], []
        for i in range(2):
            for j in range(2):
                this = amplitudes[i, j]
                combined.append((2.0 * this - amplitudes[j, i]).astype(jnp.bfloat16))
                rounded.append(this.astype(jnp.bfloat16))
                turned.append((pltpu.roll(this, BAND, 1) * sign).astype(jnp.bfloat16))
        left = jnp.concatenate(combined, axis=1)
        right = jnp.concatenate(
            [jnp.concatenate(rounded, axis=1), jnp.concatenate(turned, axis=1)], axis=0
        )
        total[slot] += lax.dot_general(
            left, right, (((1,), (1,)), ((), ())), preferred_element_type=jnp.float32
        )

    def far_step(step):
        for piece in range(per_step):
            forward(step * per_step + piece)
        shape_mate(1, step)

    def near_step(step):
        for piece in range(per_step):
            near_copy(step * per_step + piece, False).wait_recv()
        shape_mate(0, step)

    total[...] = jnp.zeros_like(total)
    lax.fori_loop(0, steps // 2, shape_own, 0)
    far_step(0)
    energy_far().wait_recv()

    @pl.when(odd == 1)
    def _():
        energy_near(True).start()

    lax.fori_loop(steps // 2, steps, shape_own, 0)
    far_step(1)
    shape_energies()

    def main_step(step, carry):
        @pl.when(step > 1)
        def _():
            far_step(step)

        near_step(step - 1)
        phase = lax.rem(step, per_band)
        ready = jnp.logical_and(step >= per_band, jnp.logical_or(phase == 1, phase == 2))

        @pl.when(ready)
        def _():
            add_band(2 - phase, step // per_band - 1)

        return carry

    lax.fori_loop(1, steps, main_step, 0)

    def swap_copy(slot):
        return pltpu.make_async_remote_copy(
            src_ref=total.at[slot, pl.ds(pl.multiple_of(other * half, half), half), :],
            dst_ref=incoming.at[slot],
            send_sem=swap_send.at[slot], recv_sem=swap_recv.at[slot],
            device_id=(me, other), device_id_type=mesh_id,
        )

    add_band(1, bands - 1)
    swap_copy(1).start()
    near_step(steps - 1)
    add_band(0, bands - 1)
    swap_copy(0).start()

    def drain(piece, carry):
        far_copy(piece).wait_send()
        near_copy(piece, False).wait_send()
        return carry

    lax.fori_loop(0, pieces, drain, 0)
    energy_far().wait_send()
    energy_near(False).wait_send()
    for slot in (1, 0):
        swap_copy(slot).wait()

    here = pl.ds(pl.multiple_of(core * half, half), half)
    for momentum in range(2):
        value = jnp.zeros((half, 2 * virtuals), jnp.float32)
        for slot in (1, 0):
            value += jnp.where(chosen[slot] == momentum, total[slot, here, :], incoming[slot])
        for part in range(2):
            out_ref[momentum, :, part, :] = value[:, part * virtuals : (part + 1) * virtuals]


def fused(factors, occupied_energy, virtual_energy, conserve, pair_lists):
    momenta, orbitals, virtuals, parts, auxiliary = factors.shape
    ring = lax.axis_size("ka")
    pieces = virtuals // PIECE
    bands = virtuals // BAND
    dma = pltpu.SemaphoreType.DMA
    return pl.pallas_call(
        functools.partial(fused_kernel, ring, virtuals, auxiliary),
        out_shape=jax.ShapeDtypeStruct((momenta, virtuals // 2, 2, virtuals), jnp.float32),
        in_specs=[
            pl.BlockSpec(memory_space=pltpu.HBM),
            pl.BlockSpec(memory_space=pltpu.HBM),
            pl.BlockSpec(memory_space=pltpu.HBM),
            pl.BlockSpec(memory_space=pltpu.HBM),
        ],
        out_specs=pl.BlockSpec(memory_space=pltpu.VMEM),
        scratch_shapes=[
            pltpu.SMEM(conserve.shape, conserve.dtype),
            pltpu.SMEM(occupied_energy.shape, occupied_energy.dtype),
            pltpu.VMEM(virtual_energy.shape, virtual_energy.dtype),
            pltpu.VMEM((momenta, orbitals, virtuals, parts, auxiliary), jnp.bfloat16),
            pltpu.VMEM((2, orbitals, virtuals, parts, auxiliary), jnp.bfloat16),
            pltpu.VMEM((momenta, orbitals * virtuals, parts * auxiliary), jnp.bfloat16),
            pltpu.VMEM((2, bands, orbitals * 2 * BAND, parts * auxiliary), jnp.bfloat16),
            pltpu.VMEM((2, momenta, virtuals), jnp.bfloat16),
            pltpu.VMEM((momenta, virtuals, LANES), jnp.float32),
            pltpu.VMEM((2, bands, 8, LANES), jnp.float32),
            pltpu.VMEM((orbitals * virtuals, orbitals * 2 * BAND), jnp.float32),
            pltpu.VMEM((2, virtuals, 2 * virtuals), jnp.float32),
            pltpu.VMEM((2, virtuals // 2, 2 * virtuals), jnp.float32),
            dma((3,)), dma((2,)),
            dma((pieces,)), dma((pieces,)), dma((pieces,)), dma((pieces,)),
            dma((2,)), dma((2,)), dma((2,)), dma((2,)),
        ],
        compiler_params=pltpu.CompilerParams(
            collective_id=0, has_side_effects=True, vmem_limit_bytes=22 * 1024 * 1024
        ),
        name="density",
    )(conserve, occupied_energy, virtual_energy, factors)


def local(factors, occupied_energy, virtual_energy, conserve, pair_lists):
    momenta, orbitals, virtuals, parts, auxiliary = factors.shape
    rounds, pairs = pair_lists.shape[:2]
    ring, holders = lax.axis_size("ka"), lax.axis_size("occ")
    whole_square = pairs * holders == orbitals * orbitals
    fits = momenta == 2 and orbitals == 2 and holders == 2 and rounds == 2
    even = ring % 2 == 0 and ring > 4 and virtuals % BAND == 0 and auxiliary % LANES == 0
    chosen = fused if whole_square and fits and even else general
    return chosen(factors, occupied_energy, virtual_energy, conserve, pair_lists)


def solution(mesh):
    in_specs = (
        P("ka", None, None, None, None),
        P(),
        P("ka", None),
        P("ka", None),
        P(None, "occ", None),
    )
    out_specs = P("ka", "occ", None, None)
    return jax.shard_map(local, mesh=mesh, in_specs=in_specs, out_specs=out_specs, check_vma=False)
```

```python
import functools

import jax
import jax.numpy as jnp
from jax import lax
from jax.experimental import pallas as pl
from jax.experimental.pallas import tpu as pltpu
from jax.sharding import PartitionSpec as P

LANES = 128
BAND = 64
STEP = 16
PIECE = 4


def from_behind(array, axis, by):
    size = lax.axis_size(axis)
    return lax.ppermute(array, axis, [(i, (i + by) % size) for i in range(size)])


def build_mates(received, auxiliary):
    real_part = received[..., :auxiliary]
    imaginary = received[..., auxiliary:]
    turned = jnp.concatenate([-imaginary, real_part], axis=-1)
    return jnp.concatenate([received, turned], axis=-2)


def amplitude(left_rows, mate_rows, energy_left, energy_right, occupied_sum):
    values = lax.dot_general(
        left_rows, mate_rows, (((1,), (1,)), ((), ())), preferred_element_type=jnp.float32
    )
    denominator = energy_left[:, None] + energy_right[None, :] - occupied_sum
    return values / jnp.concatenate([denominator, denominator], axis=1)


def density_term(amplitudes, swapped):
    virtuals = amplitudes.shape[0]
    combined = (2.0 * amplitudes - swapped).astype(jnp.bfloat16)
    rounded = amplitudes.astype(jnp.bfloat16)
    turned = jnp.concatenate([-rounded[:, virtuals:], rounded[:, :virtuals]], axis=1)
    stacked = jnp.concatenate([rounded, turned], axis=0)
    return lax.dot_general(
        combined, stacked, (((1,), (1,)), ((), ())), preferred_element_type=jnp.float32
    )


def pair_term(own_block, mate_block, energy_left, energy_right, occupied_energy, pair_row):
    leading = pair_row[0]
    trailing = pair_row[1]
    occupied_sum = occupied_energy[leading] + occupied_energy[trailing]
    amplitudes = amplitude(
        own_block[leading], mate_block[trailing], energy_left, energy_right, occupied_sum
    )
    swapped = amplitude(
        own_block[trailing], mate_block[leading], energy_left, energy_right, occupied_sum
    )
    return density_term(amplitudes, swapped)


def general(factors, occupied_energy, virtual_energy, conserve, pair_lists):
    momenta = factors.shape[0]
    orbitals = factors.shape[1]
    virtuals = factors.shape[2]
    auxiliary = factors.shape[4]
    own = factors.reshape(momenta, orbitals, virtuals, 2 * auxiliary)
    energy_own = virtual_energy.astype(jnp.float32)
    density = jnp.zeros((momenta, virtuals, 2 * virtuals), jnp.float32)
    for round_index in range(conserve.shape[1]):
        portion = orbitals // lax.axis_size("occ")
        portion_block = lax.dynamic_slice_in_dim(
            factors, lax.axis_index("occ") * portion, portion, 1
        )
        shifted, energy_mate = from_behind((portion_block, virtual_energy), "ka", round_index + 1)
        received = lax.all_gather(shifted, "occ", axis=1, tiled=True)
        mates = build_mates(received.reshape(momenta, orbitals, virtuals, 2 * auxiliary), auxiliary)
        energy_mate = energy_mate.astype(jnp.float32)
        for local_index in range(momenta):
            chosen = (momenta - conserve[local_index, round_index] % momenta) % momenta
            mate_block = lax.dynamic_index_in_dim(mates, chosen, 0, keepdims=False)
            energy_right = lax.dynamic_index_in_dim(energy_mate, chosen, 0, keepdims=False)
            own_block = own[local_index]
            energy_left = energy_own[local_index]

            def add_pair(partial_sum, pair_row):
                term = pair_term(
                    own_block, mate_block, energy_left, energy_right, occupied_energy, pair_row
                )
                return (partial_sum + term, None)

            running, ignored = lax.scan(add_pair, density[local_index], pair_lists[round_index])
            density = density.at[local_index].set(running)
    shaped = density.reshape(momenta, virtuals, 2, virtuals)
    return lax.psum_scatter(shaped, "occ", scatter_dimension=1, tiled=True)


def fused_kernel(
    ring, virtuals, auxiliary,
    conserve_hbm, occupied_hbm, energy_hbm, factors_ref, out_ref,
    conserve_ref, occupied_ref, energy_ref, own_raw, mate_raw, own, mate, energy_in, energy_left, inverse, products, total, incoming, partial,
    small_sem, own_sem, far_send, far_recv, near_send, near_recv,
    energy_send, energy_recv, swap_send, swap_recv,
):
    mesh_id = pl.DeviceIdType.MESH
    me = lax.axis_index("ka")
    core = lax.axis_index("occ")
    other = 1 - core
    odd = lax.rem(me, 2)
    half = virtuals // 2
    pieces = virtuals // PIECE
    steps = virtuals // STEP
    bands = virtuals // BAND
    per_step = STEP // PIECE
    per_band = BAND // STEP

    def at(step):
        return lax.rem(me + step + ring, ring)

    near = at(1 - 2 * odd)

    def own_copy(momentum, index):
        return pltpu.make_async_copy(
            factors_ref.at[momentum], own_raw.at[momentum], own_sem.at[index]
        )

    def small_copies():
        return (
            pltpu.make_async_copy(conserve_hbm, conserve_ref, small_sem.at[0]),
            pltpu.make_async_copy(occupied_hbm, occupied_ref, small_sem.at[1]),
            pltpu.make_async_copy(energy_hbm, energy_ref, small_sem.at[2]),
        )

    barrier = pltpu.get_barrier_semaphore()
    for place in ((at(-2), core), (near, core), (me, other)):
        pl.semaphore_signal(barrier, inc=1, device_id=place, device_id_type=mesh_id)
    own_copy(core, 0).start()
    for copy in small_copies():
        copy.start()
    own_copy(other, 1).start()

    def piece_rows(piece):
        return pl.ds(pl.multiple_of(piece * PIECE, PIECE), PIECE)

    def step_rows(step):
        return pl.ds(pl.multiple_of(step * STEP, STEP), STEP)

    def far_copy(piece):
        return pltpu.make_async_remote_copy(
            src_ref=own_raw.at[core, :, piece_rows(piece)],
            dst_ref=mate_raw.at[1, :, piece_rows(piece)],
            send_sem=far_send.at[piece], recv_sem=far_recv.at[piece],
            device_id=(at(2), core), device_id_type=mesh_id,
        )

    def near_copy(piece, relay):
        source = mate_raw.at[1] if relay else own_raw.at[core]
        return pltpu.make_async_remote_copy(
            src_ref=source.at[:, piece_rows(piece)],
            dst_ref=mate_raw.at[0, :, piece_rows(piece)],
            send_sem=near_send.at[piece], recv_sem=near_recv.at[piece],
            device_id=(near, core), device_id_type=mesh_id,
        )

    def energy_far():
        return pltpu.make_async_remote_copy(
            src_ref=energy_ref, dst_ref=energy_in.at[1],
            send_sem=energy_send.at[1], recv_sem=energy_recv.at[1],
            device_id=(at(2), core), device_id_type=mesh_id,
        )

    def energy_near(relay):
        return pltpu.make_async_remote_copy(
            src_ref=energy_in.at[1] if relay else energy_ref, dst_ref=energy_in.at[0],
            send_sem=energy_send.at[0], recv_sem=energy_recv.at[0],
            device_id=(near, core), device_id_type=mesh_id,
        )

    own_copy(core, 0).wait()
    pl.semaphore_wait(barrier, 3)

    def send_piece(piece, carry):
        far_copy(piece).start()

        @pl.when(odd == 0)
        def _():
            near_copy(piece, False).start()

        return carry

    lax.fori_loop(0, 2, send_piece, 0)
    for copy in small_copies():
        copy.wait()
    energy_far().start()

    @pl.when(odd == 0)
    def _():
        energy_near(False).start()

    lax.fori_loop(2, pieces, send_piece, 0)

    chosen = []
    for slot in range(2):
        mirror = lax.rem(2 - lax.rem(conserve_ref[0, slot], 2), 2)
        chosen.append(jnp.where(mirror == core, 0, 1))

    own_copy(other, 1).wait()

    def forward(piece):
        far_copy(piece).wait_recv()

        @pl.when(odd == 1)
        def _():
            near_copy(piece, True).start()

    def shape_own(step, carry):
        for momentum in range(2):
            for orbital in range(2):
                row = pl.ds(pl.multiple_of(orbital * virtuals + step * STEP, STEP), STEP)
                for part in range(2):
                    own[momentum, row, pl.ds(part * auxiliary, auxiliary)] = own_raw[
                        momentum, orbital, step_rows(step), part, :
                    ]
        return carry

    def shape_mate(slot, step):
        band = step // per_band
        for orbital in range(2):
            real = mate_raw[slot, orbital, step_rows(step), 0, :]
            imaginary = mate_raw[slot, orbital, step_rows(step), 1, :]
            first = orbital * 2 * BAND + lax.rem(step, per_band) * STEP
            plain = pl.ds(pl.multiple_of(first, STEP), STEP)
            turned = pl.ds(pl.multiple_of(first + BAND, STEP), STEP)
            mate[slot, band, plain, pl.ds(0, auxiliary)] = real
            mate[slot, band, plain, pl.ds(auxiliary, auxiliary)] = imaginary
            mate[slot, band, turned, pl.ds(0, auxiliary)] = -imaginary
            mate[slot, band, turned, pl.ds(auxiliary, auxiliary)] = real

    def shape_energies():
        sums = [occupied_ref[0] + occupied_ref[0], occupied_ref[0] + occupied_ref[1]]
        sums.append(occupied_ref[1] + occupied_ref[1])
        diagonal = lax.broadcasted_iota(
            jnp.int32, (virtuals, virtuals), 0
        ) == lax.broadcasted_iota(jnp.int32, (virtuals, virtuals), 1)
        mine = energy_ref[...].astype(jnp.float32)
        for momentum in range(2):
            spread = jnp.where(diagonal, mine[momentum : momentum + 1, :], 0.0)
            column = jnp.sum(spread, axis=1, keepdims=True)
            energy_left[momentum] = jnp.broadcast_to(column, (virtuals, LANES))
        energy_near(False).wait_recv()
        for slot in range(2):
            theirs = energy_in[slot].astype(jnp.float32)
            theirs = jnp.where(core == 0, theirs[0:1, :], theirs[1:2, :])
            for band in range(bands):
                part = theirs[:, band * BAND : (band + 1) * BAND]
                row = jnp.concatenate([part, part], axis=1)
                base = energy_left[chosen[slot]] + row
                for kind in range(3):
                    inverse[slot, band, kind] = 1.0 / (base - sums[kind])

    sign = jnp.where(lax.broadcasted_iota(jnp.int32, (virtuals, LANES), 1) < BAND, -1.0, 1.0)

    def add_band(slot, band):
        momentum = jnp.where(slot == 1, chosen[1], chosen[0])
        products[...] = lax.dot_general(
            own[momentum], mate[slot, band], (((1,), (1,)), ((), ())),
            preferred_element_type=jnp.float32,
        )
        amplitudes = {}
        for i in range(2):
            for j in range(2):
                value = products[i * virtuals : (i + 1) * virtuals, j * LANES : (j + 1) * LANES]
                amplitudes[i, j] = value * inverse[slot, band, i + j]
        combined, rounded, turned = [], [], []
        for i in range(2):
            for j in range(2):
                this = amplitudes[i, j]
                combined.append((2.0 * this - amplitudes[j, i]).astype(jnp.bfloat16))
                rounded.append(this.astype(jnp.bfloat16))
                turned.append((pltpu.roll(this, BAND, 1) * sign).astype(jnp.bfloat16))
        left = jnp.concatenate(combined, axis=1)
        right = jnp.concatenate(
            [jnp.concatenate(rounded, axis=1), jnp.concatenate(turned, axis=1)], axis=0
        )
        total[slot] += lax.dot_general(
            left, right, (((1,), (1,)), ((), ())), preferred_element_type=jnp.float32
        )

    def far_step(step):
        for piece in range(per_step):
            forward(step * per_step + piece)
        shape_mate(1, step)

    def near_step(step):
        for piece in range(per_step):
            near_copy(step * per_step + piece, False).wait_recv()
        shape_mate(0, step)

    total[...] = jnp.zeros_like(total)
    lax.fori_loop(0, steps // 2, shape_own, 0)
    far_step(0)
    energy_far().wait_recv()

    @pl.when(odd == 1)
    def _():
        energy_near(True).start()

    lax.fori_loop(steps // 2, steps, shape_own, 0)
    far_step(1)
    shape_energies()

    def main_step(step, carry):
        @pl.when(step > 1)
        def _():
            far_step(step)

        near_step(step - 1)
        phase = lax.rem(step, per_band)
        ready = jnp.logical_and(step >= per_band, jnp.logical_or(phase == 1, phase == 2))

        @pl.when(ready)
        def _():
            add_band(2 - phase, step // per_band - 1)

        return carry

    lax.fori_loop(1, steps, main_step, 0)

    def swap_copy(slot):
        return pltpu.make_async_remote_copy(
            src_ref=total.at[slot, pl.ds(pl.multiple_of(other * half, half), half), :],
            dst_ref=incoming.at[slot],
            send_sem=swap_send.at[slot], recv_sem=swap_recv.at[slot],
            device_id=(me, other), device_id_type=mesh_id,
        )

    add_band(1, bands - 1)
    swap_copy(1).start()
    near_step(steps - 1)
    add_band(0, bands - 1)
    swap_copy(0).start()

    def drain(piece, carry):
        far_copy(piece).wait_send()
        near_copy(piece, False).wait_send()
        return carry

    lax.fori_loop(0, pieces, drain, 0)
    energy_far().wait_send()
    energy_near(False).wait_send()
    here = pl.ds(pl.multiple_of(core * half, half), half)
    swap_copy(1).wait()
    for momentum in range(2):
        known = jnp.where(chosen[1] == momentum, total[1, here, :], incoming[1])
        partial[momentum] = known + jnp.where(chosen[0] == momentum, total[0, here, :], 0.0)
    swap_copy(0).wait()
    for momentum in range(2):
        value = partial[momentum] + jnp.where(chosen[0] == momentum, 0.0, incoming[0])
        for part in range(2):
            out_ref[momentum, :, part, :] = value[:, part * virtuals : (part + 1) * virtuals]


def fused(factors, occupied_energy, virtual_energy, conserve, pair_lists):
    momenta, orbitals, virtuals, parts, auxiliary = factors.shape
    ring = lax.axis_size("ka")
    pieces = virtuals // PIECE
    bands = virtuals // BAND
    dma = pltpu.SemaphoreType.DMA
    return pl.pallas_call(
        functools.partial(fused_kernel, ring, virtuals, auxiliary),
        out_shape=jax.ShapeDtypeStruct((momenta, virtuals // 2, 2, virtuals), jnp.float32),
        in_specs=[
            pl.BlockSpec(memory_space=pltpu.HBM),
            pl.BlockSpec(memory_space=pltpu.HBM),
            pl.BlockSpec(memory_space=pltpu.HBM),
            pl.BlockSpec(memory_space=pltpu.HBM),
        ],
        out_specs=pl.BlockSpec(memory_space=pltpu.VMEM),
        scratch_shapes=[
            pltpu.SMEM(conserve.shape, conserve.dtype),
            pltpu.SMEM(occupied_energy.shape, occupied_energy.dtype),
            pltpu.VMEM(virtual_energy.shape, virtual_energy.dtype),
            pltpu.VMEM((momenta, orbitals, virtuals, parts, auxiliary), jnp.bfloat16),
            pltpu.VMEM((2, orbitals, virtuals, parts, auxiliary), jnp.bfloat16),
            pltpu.VMEM((momenta, orbitals * virtuals, parts * auxiliary), jnp.bfloat16),
            pltpu.VMEM((2, bands, orbitals * 2 * BAND, parts * auxiliary), jnp.bfloat16),
            pltpu.VMEM((2, momenta, virtuals), jnp.bfloat16),
            pltpu.VMEM((momenta, virtuals, LANES), jnp.float32),
            pltpu.VMEM((2, bands, 3, virtuals, LANES), jnp.float32),
            pltpu.VMEM((orbitals * virtuals, orbitals * 2 * BAND), jnp.float32),
            pltpu.VMEM((2, virtuals, 2 * virtuals), jnp.float32),
            pltpu.VMEM((2, virtuals // 2, 2 * virtuals), jnp.float32),
            pltpu.VMEM((2, virtuals // 2, 2 * virtuals), jnp.float32),
            dma((3,)), dma((2,)),
            dma((pieces,)), dma((pieces,)), dma((pieces,)), dma((pieces,)),
            dma((2,)), dma((2,)), dma((2,)), dma((2,)),
        ],
        compiler_params=pltpu.CompilerParams(
            collective_id=0, has_side_effects=True, vmem_limit_bytes=54 * 1024 * 1024
        ),
        name="density",
    )(conserve, occupied_energy, virtual_energy, factors)


def local(factors, occupied_energy, virtual_energy, conserve, pair_lists):
    momenta, orbitals, virtuals, parts, auxiliary = factors.shape
    rounds, pairs = pair_lists.shape[:2]
    ring, holders = lax.axis_size("ka"), lax.axis_size("occ")
    whole_square = pairs * holders == orbitals * orbitals
    fits = momenta == 2 and orbitals == 2 and holders == 2 and rounds == 2
    even = ring % 2 == 0 and ring > 4 and virtuals % BAND == 0 and auxiliary % LANES == 0
    chosen = fused if whole_square and fits and even else general
    return chosen(factors, occupied_energy, virtual_energy, conserve, pair_lists)


def solution(mesh):
    in_specs = (
        P("ka", None, None, None, None),
        P(),
        P("ka", None),
        P("ka", None),
        P(None, "occ", None),
    )
    out_specs = P("ka", "occ", None, None)
    return jax.shard_map(local, mesh=mesh, in_specs=in_specs, out_specs=out_specs, check_vma=False)
```

```python
import functools

import jax
import jax.numpy as jnp
from jax import lax
from jax.experimental import pallas as pl
from jax.experimental.pallas import tpu as pltpu
from jax.sharding import PartitionSpec as P

LANES = 128
BAND = 64
STEP = 16
PIECE = 4


def from_behind(array, axis, by):
    size = lax.axis_size(axis)
    return lax.ppermute(array, axis, [(i, (i + by) % size) for i in range(size)])


def build_mates(received, auxiliary):
    real_part = received[..., :auxiliary]
    imaginary = received[..., auxiliary:]
    turned = jnp.concatenate([-imaginary, real_part], axis=-1)
    return jnp.concatenate([received, turned], axis=-2)


def amplitude(left_rows, mate_rows, energy_left, energy_right, occupied_sum):
    values = lax.dot_general(
        left_rows, mate_rows, (((1,), (1,)), ((), ())), preferred_element_type=jnp.float32
    )
    denominator = energy_left[:, None] + energy_right[None, :] - occupied_sum
    return values / jnp.concatenate([denominator, denominator], axis=1)


def density_term(amplitudes, swapped):
    virtuals = amplitudes.shape[0]
    combined = (2.0 * amplitudes - swapped).astype(jnp.bfloat16)
    rounded = amplitudes.astype(jnp.bfloat16)
    turned = jnp.concatenate([-rounded[:, virtuals:], rounded[:, :virtuals]], axis=1)
    stacked = jnp.concatenate([rounded, turned], axis=0)
    return lax.dot_general(
        combined, stacked, (((1,), (1,)), ((), ())), preferred_element_type=jnp.float32
    )


def pair_term(own_block, mate_block, energy_left, energy_right, occupied_energy, pair_row):
    leading = pair_row[0]
    trailing = pair_row[1]
    occupied_sum = occupied_energy[leading] + occupied_energy[trailing]
    amplitudes = amplitude(
        own_block[leading], mate_block[trailing], energy_left, energy_right, occupied_sum
    )
    swapped = amplitude(
        own_block[trailing], mate_block[leading], energy_left, energy_right, occupied_sum
    )
    return density_term(amplitudes, swapped)


def general(factors, occupied_energy, virtual_energy, conserve, pair_lists):
    momenta = factors.shape[0]
    orbitals = factors.shape[1]
    virtuals = factors.shape[2]
    auxiliary = factors.shape[4]
    own = factors.reshape(momenta, orbitals, virtuals, 2 * auxiliary)
    energy_own = virtual_energy.astype(jnp.float32)
    density = jnp.zeros((momenta, virtuals, 2 * virtuals), jnp.float32)
    for round_index in range(conserve.shape[1]):
        portion = orbitals // lax.axis_size("occ")
        portion_block = lax.dynamic_slice_in_dim(
            factors, lax.axis_index("occ") * portion, portion, 1
        )
        shifted, energy_mate = from_behind((portion_block, virtual_energy), "ka", round_index + 1)
        received = lax.all_gather(shifted, "occ", axis=1, tiled=True)
        mates = build_mates(received.reshape(momenta, orbitals, virtuals, 2 * auxiliary), auxiliary)
        energy_mate = energy_mate.astype(jnp.float32)
        for local_index in range(momenta):
            chosen = (momenta - conserve[local_index, round_index] % momenta) % momenta
            mate_block = lax.dynamic_index_in_dim(mates, chosen, 0, keepdims=False)
            energy_right = lax.dynamic_index_in_dim(energy_mate, chosen, 0, keepdims=False)
            own_block = own[local_index]
            energy_left = energy_own[local_index]

            def add_pair(partial_sum, pair_row):
                term = pair_term(
                    own_block, mate_block, energy_left, energy_right, occupied_energy, pair_row
                )
                return (partial_sum + term, None)

            running, ignored = lax.scan(add_pair, density[local_index], pair_lists[round_index])
            density = density.at[local_index].set(running)
    shaped = density.reshape(momenta, virtuals, 2, virtuals)
    return lax.psum_scatter(shaped, "occ", scatter_dimension=1, tiled=True)


def fused_kernel(
    ring, virtuals, auxiliary,
    conserve_hbm, occupied_hbm, energy_hbm, factors_ref, out_ref,
    conserve_ref, occupied_ref, energy_ref, own_raw, mate_raw, own, mate, energy_in, energy_left, inverse, products, total, incoming, partial,
    small_sem, own_sem, far_send, far_recv, near_send, near_recv,
    energy_send, energy_recv, swap_send, swap_recv,
):
    mesh_id = pl.DeviceIdType.MESH
    me = lax.axis_index("ka")
    core = lax.axis_index("occ")
    other = 1 - core
    odd = lax.rem(me, 2)
    half = virtuals // 2
    pieces = virtuals // PIECE
    steps = virtuals // STEP
    bands = virtuals // BAND
    per_step = STEP // PIECE
    per_band = BAND // STEP

    def at(step):
        return lax.rem(me + step + ring, ring)

    near = at(1 - 2 * odd)

    def own_copy(momentum, index):
        return pltpu.make_async_copy(
            factors_ref.at[momentum], own_raw.at[momentum], own_sem.at[index]
        )

    def small_copies():
        return (
            pltpu.make_async_copy(conserve_hbm, conserve_ref, small_sem.at[0]),
            pltpu.make_async_copy(occupied_hbm, occupied_ref, small_sem.at[1]),
            pltpu.make_async_copy(energy_hbm, energy_ref, small_sem.at[2]),
        )

    barrier = pltpu.get_barrier_semaphore()
    for place in ((at(-2), core), (near, core), (me, other)):
        pl.semaphore_signal(barrier, inc=1, device_id=place, device_id_type=mesh_id)
    own_copy(core, 0).start()
    for copy in small_copies():
        copy.start()
    own_copy(other, 1).start()

    def piece_rows(piece):
        return pl.ds(pl.multiple_of(piece * PIECE, PIECE), PIECE)

    def step_rows(step):
        return pl.ds(pl.multiple_of(step * STEP, STEP), STEP)

    def far_copy(piece):
        return pltpu.make_async_remote_copy(
            src_ref=own_raw.at[core, :, piece_rows(piece)],
            dst_ref=mate_raw.at[1, :, piece_rows(piece)],
            send_sem=far_send.at[piece], recv_sem=far_recv.at[piece],
            device_id=(at(2), core), device_id_type=mesh_id,
        )

    def near_copy(piece, relay):
        source = mate_raw.at[1] if relay else own_raw.at[core]
        return pltpu.make_async_remote_copy(
            src_ref=source.at[:, piece_rows(piece)],
            dst_ref=mate_raw.at[0, :, piece_rows(piece)],
            send_sem=near_send.at[piece], recv_sem=near_recv.at[piece],
            device_id=(near, core), device_id_type=mesh_id,
        )

    def energy_far():
        return pltpu.make_async_remote_copy(
            src_ref=energy_ref, dst_ref=energy_in.at[1],
            send_sem=energy_send.at[1], recv_sem=energy_recv.at[1],
            device_id=(at(2), core), device_id_type=mesh_id,
        )

    def energy_near(relay):
        return pltpu.make_async_remote_copy(
            src_ref=energy_in.at[1] if relay else energy_ref, dst_ref=energy_in.at[0],
            send_sem=energy_send.at[0], recv_sem=energy_recv.at[0],
            device_id=(near, core), device_id_type=mesh_id,
        )

    own_copy(core, 0).wait()
    pl.semaphore_wait(barrier, 3)

    def send_piece(piece, carry):
        far_copy(piece).start()

        @pl.when(odd == 0)
        def _():
            near_copy(piece, False).start()

        return carry

    lax.fori_loop(0, 2, send_piece, 0)
    for copy in small_copies():
        copy.wait()
    energy_far().start()

    @pl.when(odd == 0)
    def _():
        energy_near(False).start()

    lax.fori_loop(2, pieces, send_piece, 0)

    chosen = []
    for slot in range(2):
        mirror = lax.rem(2 - lax.rem(conserve_ref[0, slot], 2), 2)
        chosen.append(jnp.where(mirror == core, 0, 1))

    own_copy(other, 1).wait()

    def forward(piece):
        far_copy(piece).wait_recv()

        @pl.when(odd == 1)
        def _():
            near_copy(piece, True).start()

    def shape_own(step, carry):
        for momentum in range(2):
            for orbital in range(2):
                row = pl.ds(pl.multiple_of(orbital * virtuals + step * STEP, STEP), STEP)
                for part in range(2):
                    own[momentum, row, pl.ds(part * auxiliary, auxiliary)] = own_raw[
                        momentum, orbital, step_rows(step), part, :
                    ]
        return carry

    def shape_mate(slot, step):
        band = step // per_band
        for orbital in range(2):
            real = mate_raw[slot, orbital, step_rows(step), 0, :]
            imaginary = mate_raw[slot, orbital, step_rows(step), 1, :]
            first = orbital * 2 * BAND + lax.rem(step, per_band) * STEP
            plain = pl.ds(pl.multiple_of(first, STEP), STEP)
            turned = pl.ds(pl.multiple_of(first + BAND, STEP), STEP)
            mate[slot, band, plain, pl.ds(0, auxiliary)] = real
            mate[slot, band, plain, pl.ds(auxiliary, auxiliary)] = imaginary
            mate[slot, band, turned, pl.ds(0, auxiliary)] = -imaginary
            mate[slot, band, turned, pl.ds(auxiliary, auxiliary)] = real

    def shape_energies():
        sums = [occupied_ref[0] + occupied_ref[0], occupied_ref[0] + occupied_ref[1]]
        sums.append(occupied_ref[1] + occupied_ref[1])
        diagonal = lax.broadcasted_iota(
            jnp.int32, (virtuals, virtuals), 0
        ) == lax.broadcasted_iota(jnp.int32, (virtuals, virtuals), 1)
        mine = energy_ref[...].astype(jnp.float32)
        for momentum in range(2):
            spread = jnp.where(diagonal, mine[momentum : momentum + 1, :], 0.0)
            column = jnp.sum(spread, axis=1, keepdims=True)
            energy_left[momentum] = jnp.broadcast_to(column, (virtuals, LANES))
        energy_near(False).wait_recv()
        for slot in range(2):
            theirs = energy_in[slot].astype(jnp.float32)
            theirs = jnp.where(core == 0, theirs[0:1, :], theirs[1:2, :])
            for band in range(bands):
                part = theirs[:, band * BAND : (band + 1) * BAND]
                row = jnp.concatenate([part, part], axis=1)
                base = energy_left[chosen[slot]] + row
                for kind in range(3):
                    inverse[slot, band, kind] = 1.0 / (base - sums[kind])

    sign = jnp.where(lax.broadcasted_iota(jnp.int32, (virtuals, LANES), 1) < BAND, -1.0, 1.0)

    def add_band(slot, band):
        momentum = jnp.where(slot == 1, chosen[1], chosen[0])
        products[...] = lax.dot_general(
            own[momentum], mate[slot, band], (((1,), (1,)), ((), ())),
            preferred_element_type=jnp.float32,
        )
        amplitudes = {}
        for i in range(2):
            for j in range(2):
                value = products[i * virtuals : (i + 1) * virtuals, j * LANES : (j + 1) * LANES]
                amplitudes[i, j] = value * inverse[slot, band, i + j]
        combined, rounded, turned = [], [], []
        for i in range(2):
            for j in range(2):
                this = amplitudes[i, j]
                combined.append((2.0 * this - amplitudes[j, i]).astype(jnp.bfloat16))
                rounded.append(this.astype(jnp.bfloat16))
                turned.append((pltpu.roll(this, BAND, 1) * sign).astype(jnp.bfloat16))
        left = jnp.concatenate(combined, axis=1)
        right = jnp.concatenate(
            [jnp.concatenate(rounded, axis=1), jnp.concatenate(turned, axis=1)], axis=0
        )
        total[slot] += lax.dot_general(
            left, right, (((1,), (1,)), ((), ())), preferred_element_type=jnp.float32
        )

    def far_step(step):
        for piece in range(per_step):
            forward(step * per_step + piece)
        shape_mate(1, step)

    def near_step(step):
        for piece in range(per_step):
            near_copy(step * per_step + piece, False).wait_recv()
        shape_mate(0, step)

    total[...] = jnp.zeros_like(total)
    lax.fori_loop(0, steps // 2, shape_own, 0)
    far_step(0)
    energy_far().wait_recv()

    @pl.when(odd == 1)
    def _():
        energy_near(True).start()

    lax.fori_loop(steps // 2, steps, shape_own, 0)
    far_step(1)
    shape_energies()

    def main_step(step, carry):
        @pl.when(step > 1)
        def _():
            far_step(step)

        near_step(step - 1)
        phase = lax.rem(step, per_band)
        ready = jnp.logical_and(step >= per_band, jnp.logical_or(phase == 1, phase == 2))

        @pl.when(ready)
        def _():
            add_band(2 - phase, step // per_band - 1)

        return carry

    lax.fori_loop(1, steps, main_step, 0)

    def swap_copy(slot):
        return pltpu.make_async_remote_copy(
            src_ref=total.at[slot, pl.ds(pl.multiple_of(other * half, half), half), :],
            dst_ref=incoming.at[slot],
            send_sem=swap_send.at[slot], recv_sem=swap_recv.at[slot],
            device_id=(me, other), device_id_type=mesh_id,
        )

    add_band(1, bands - 1)
    swap_copy(1).start()
    near_step(steps - 1)
    add_band(0, bands - 1)
    swap_copy(0).start()

    def drain(piece, carry):
        far_copy(piece).wait_send()
        near_copy(piece, False).wait_send()
        return carry

    lax.fori_loop(0, pieces, drain, 0)
    energy_far().wait_send()
    energy_near(False).wait_send()
    here = pl.ds(pl.multiple_of(core * half, half), half)
    swap_copy(1).wait()
    for momentum in range(2):
        known = jnp.where(chosen[1] == momentum, total[1, here, :], incoming[1])
        partial[momentum] = known + jnp.where(chosen[0] == momentum, total[0, here, :], 0.0)
    swap_copy(0).wait()
    for momentum in range(2):
        value = partial[momentum] + jnp.where(chosen[0] == momentum, 0.0, incoming[0])
        for part in range(2):
            out_ref[momentum, :, part, :] = value[:, part * virtuals : (part + 1) * virtuals]


def fused(factors, occupied_energy, virtual_energy, conserve, pair_lists):
    momenta, orbitals, virtuals, parts, auxiliary = factors.shape
    ring = lax.axis_size("ka")
    pieces = virtuals // PIECE
    bands = virtuals // BAND
    dma = pltpu.SemaphoreType.DMA
    return pl.pallas_call(
        functools.partial(fused_kernel, ring, virtuals, auxiliary),
        out_shape=pltpu.VMEM((momenta, virtuals // 2, 2, virtuals), jnp.float32),
        in_specs=[
            pl.BlockSpec(memory_space=pltpu.HBM),
            pl.BlockSpec(memory_space=pltpu.HBM),
            pl.BlockSpec(memory_space=pltpu.HBM),
            pl.BlockSpec(memory_space=pltpu.HBM),
        ],
        out_specs=pl.BlockSpec(memory_space=pltpu.VMEM),
        scratch_shapes=[
            pltpu.SMEM(conserve.shape, conserve.dtype),
            pltpu.SMEM(occupied_energy.shape, occupied_energy.dtype),
            pltpu.VMEM(virtual_energy.shape, virtual_energy.dtype),
            pltpu.VMEM((momenta, orbitals, virtuals, parts, auxiliary), jnp.bfloat16),
            pltpu.VMEM((2, orbitals, virtuals, parts, auxiliary), jnp.bfloat16),
            pltpu.VMEM((momenta, orbitals * virtuals, parts * auxiliary), jnp.bfloat16),
            pltpu.VMEM((2, bands, orbitals * 2 * BAND, parts * auxiliary), jnp.bfloat16),
            pltpu.VMEM((2, momenta, virtuals), jnp.bfloat16),
            pltpu.VMEM((momenta, virtuals, LANES), jnp.float32),
            pltpu.VMEM((2, bands, 3, virtuals, LANES), jnp.float32),
            pltpu.VMEM((orbitals * virtuals, orbitals * 2 * BAND), jnp.float32),
            pltpu.VMEM((2, virtuals, 2 * virtuals), jnp.float32),
            pltpu.VMEM((2, virtuals // 2, 2 * virtuals), jnp.float32),
            pltpu.VMEM((2, virtuals // 2, 2 * virtuals), jnp.float32),
            dma((3,)), dma((2,)),
            dma((pieces,)), dma((pieces,)), dma((pieces,)), dma((pieces,)),
            dma((2,)), dma((2,)), dma((2,)), dma((2,)),
        ],
        compiler_params=pltpu.CompilerParams(
            collective_id=0, has_side_effects=True, vmem_limit_bytes=54 * 1024 * 1024
        ),
        name="density",
    )(conserve, occupied_energy, virtual_energy, factors)


def local(factors, occupied_energy, virtual_energy, conserve, pair_lists):
    momenta, orbitals, virtuals, parts, auxiliary = factors.shape
    rounds, pairs = pair_lists.shape[:2]
    ring, holders = lax.axis_size("ka"), lax.axis_size("occ")
    whole_square = pairs * holders == orbitals * orbitals
    fits = momenta == 2 and orbitals == 2 and holders == 2 and rounds == 2
    even = ring % 2 == 0 and ring > 4 and virtuals % BAND == 0 and auxiliary % LANES == 0
    chosen = fused if whole_square and fits and even else general
    return chosen(factors, occupied_energy, virtual_energy, conserve, pair_lists)


def solution(mesh):
    in_specs = (
        P("ka", None, None, None, None),
        P(),
        P("ka", None),
        P("ka", None),
        P(None, "occ", None),
    )
    out_specs = P("ka", "occ", None, None)
    return jax.shard_map(local, mesh=mesh, in_specs=in_specs, out_specs=out_specs, check_vma=False)
```

```python
import functools

import jax
import jax.numpy as jnp
from jax import lax
from jax.experimental import pallas as pl
from jax.experimental.pallas import tpu as pltpu
from jax.sharding import PartitionSpec as P

LANES = 128
BAND = 64
STEP = 16
PIECE = 8


def from_behind(array, axis, by):
    size = lax.axis_size(axis)
    return lax.ppermute(array, axis, [(i, (i + by) % size) for i in range(size)])


def build_mates(received, auxiliary):
    real_part = received[..., :auxiliary]
    imaginary = received[..., auxiliary:]
    turned = jnp.concatenate([-imaginary, real_part], axis=-1)
    return jnp.concatenate([received, turned], axis=-2)


def amplitude(left_rows, mate_rows, energy_left, energy_right, occupied_sum):
    values = lax.dot_general(
        left_rows, mate_rows, (((1,), (1,)), ((), ())), preferred_element_type=jnp.float32
    )
    denominator = energy_left[:, None] + energy_right[None, :] - occupied_sum
    return values / jnp.concatenate([denominator, denominator], axis=1)


def density_term(amplitudes, swapped):
    virtuals = amplitudes.shape[0]
    combined = (2.0 * amplitudes - swapped).astype(jnp.bfloat16)
    rounded = amplitudes.astype(jnp.bfloat16)
    turned = jnp.concatenate([-rounded[:, virtuals:], rounded[:, :virtuals]], axis=1)
    stacked = jnp.concatenate([rounded, turned], axis=0)
    return lax.dot_general(
        combined, stacked, (((1,), (1,)), ((), ())), preferred_element_type=jnp.float32
    )


def pair_term(own_block, mate_block, energy_left, energy_right, occupied_energy, pair_row):
    leading = pair_row[0]
    trailing = pair_row[1]
    occupied_sum = occupied_energy[leading] + occupied_energy[trailing]
    amplitudes = amplitude(
        own_block[leading], mate_block[trailing], energy_left, energy_right, occupied_sum
    )
    swapped = amplitude(
        own_block[trailing], mate_block[leading], energy_left, energy_right, occupied_sum
    )
    return density_term(amplitudes, swapped)


def general(factors, occupied_energy, virtual_energy, conserve, pair_lists):
    momenta = factors.shape[0]
    orbitals = factors.shape[1]
    virtuals = factors.shape[2]
    auxiliary = factors.shape[4]
    own = factors.reshape(momenta, orbitals, virtuals, 2 * auxiliary)
    energy_own = virtual_energy.astype(jnp.float32)
    density = jnp.zeros((momenta, virtuals, 2 * virtuals), jnp.float32)
    for round_index in range(conserve.shape[1]):
        portion = orbitals // lax.axis_size("occ")
        portion_block = lax.dynamic_slice_in_dim(
            factors, lax.axis_index("occ") * portion, portion, 1
        )
        shifted, energy_mate = from_behind((portion_block, virtual_energy), "ka", round_index + 1)
        received = lax.all_gather(shifted, "occ", axis=1, tiled=True)
        mates = build_mates(received.reshape(momenta, orbitals, virtuals, 2 * auxiliary), auxiliary)
        energy_mate = energy_mate.astype(jnp.float32)
        for local_index in range(momenta):
            chosen = (momenta - conserve[local_index, round_index] % momenta) % momenta
            mate_block = lax.dynamic_index_in_dim(mates, chosen, 0, keepdims=False)
            energy_right = lax.dynamic_index_in_dim(energy_mate, chosen, 0, keepdims=False)
            own_block = own[local_index]
            energy_left = energy_own[local_index]

            def add_pair(partial_sum, pair_row):
                term = pair_term(
                    own_block, mate_block, energy_left, energy_right, occupied_energy, pair_row
                )
                return (partial_sum + term, None)

            running, ignored = lax.scan(add_pair, density[local_index], pair_lists[round_index])
            density = density.at[local_index].set(running)
    shaped = density.reshape(momenta, virtuals, 2, virtuals)
    return lax.psum_scatter(shaped, "occ", scatter_dimension=1, tiled=True)


def fused_kernel(
    ring, virtuals, auxiliary,
    conserve_hbm, occupied_hbm, energy_hbm, factors_ref, out_ref,
    conserve_ref, occupied_ref, energy_ref, own_raw, mate_raw, own, mate, energy_in, energy_left, inverse, products, total, incoming, partial,
    small_sem, own_sem, far_send, far_recv, near_send, near_recv,
    energy_send, energy_recv, swap_send, swap_recv,
):
    mesh_id = pl.DeviceIdType.MESH
    me = lax.axis_index("ka")
    core = lax.axis_index("occ")
    other = 1 - core
    odd = lax.rem(me, 2)
    half = virtuals // 2
    pieces = virtuals // PIECE
    steps = virtuals // STEP
    bands = virtuals // BAND
    per_step = STEP // PIECE
    per_band = BAND // STEP

    def at(step):
        return lax.rem(me + step + ring, ring)

    near = at(1 - 2 * odd)

    def own_copy(momentum, index):
        return pltpu.make_async_copy(
            factors_ref.at[momentum], own_raw.at[momentum], own_sem.at[index]
        )

    def small_copies():
        return (
            pltpu.make_async_copy(conserve_hbm, conserve_ref, small_sem.at[0]),
            pltpu.make_async_copy(occupied_hbm, occupied_ref, small_sem.at[1]),
            pltpu.make_async_copy(energy_hbm, energy_ref, small_sem.at[2]),
        )

    barrier = pltpu.get_barrier_semaphore()
    for place in ((at(-2), core), (near, core), (me, other)):
        pl.semaphore_signal(barrier, inc=1, device_id=place, device_id_type=mesh_id)
    own_copy(core, 0).start()
    for copy in small_copies():
        copy.start()
    own_copy(other, 1).start()

    def piece_rows(piece):
        return pl.ds(pl.multiple_of(piece * PIECE, PIECE), PIECE)

    def step_rows(step):
        return pl.ds(pl.multiple_of(step * STEP, STEP), STEP)

    def far_copy(piece):
        return pltpu.make_async_remote_copy(
            src_ref=own_raw.at[core, :, piece_rows(piece)],
            dst_ref=mate_raw.at[1, :, piece_rows(piece)],
            send_sem=far_send.at[piece], recv_sem=far_recv.at[piece],
            device_id=(at(2), core), device_id_type=mesh_id,
        )

    def near_copy(piece, relay):
        source = mate_raw.at[1] if relay else own_raw.at[core]
        return pltpu.make_async_remote_copy(
            src_ref=source.at[:, piece_rows(piece)],
            dst_ref=mate_raw.at[0, :, piece_rows(piece)],
            send_sem=near_send.at[piece], recv_sem=near_recv.at[piece],
            device_id=(near, core), device_id_type=mesh_id,
        )

    def energy_far():
        return pltpu.make_async_remote_copy(
            src_ref=energy_ref, dst_ref=energy_in.at[1],
            send_sem=energy_send.at[1], recv_sem=energy_recv.at[1],
            device_id=(at(2), core), device_id_type=mesh_id,
        )

    def energy_near(relay):
        return pltpu.make_async_remote_copy(
            src_ref=energy_in.at[1] if relay else energy_ref, dst_ref=energy_in.at[0],
            send_sem=energy_send.at[0], recv_sem=energy_recv.at[0],
            device_id=(near, core), device_id_type=mesh_id,
        )

    own_copy(core, 0).wait()
    pl.semaphore_wait(barrier, 3)

    def send_piece(piece, carry):
        far_copy(piece).start()

        @pl.when(odd == 0)
        def _():
            near_copy(piece, False).start()

        return carry

    lax.fori_loop(0, 2, send_piece, 0)
    for copy in small_copies():
        copy.wait()
    energy_far().start()

    @pl.when(odd == 0)
    def _():
        energy_near(False).start()

    lax.fori_loop(2, pieces, send_piece, 0)

    chosen = []
    for slot in range(2):
        mirror = lax.rem(2 - lax.rem(conserve_ref[0, slot], 2), 2)
        chosen.append(jnp.where(mirror == core, 0, 1))

    own_copy(other, 1).wait()

    def forward(piece):
        far_copy(piece).wait_recv()

        @pl.when(odd == 1)
        def _():
            near_copy(piece, True).start()

    def shape_own(step, carry):
        for momentum in range(2):
            for orbital in range(2):
                row = pl.ds(pl.multiple_of(orbital * virtuals + step * STEP, STEP), STEP)
                for part in range(2):
                    own[momentum, row, pl.ds(part * auxiliary, auxiliary)] = own_raw[
                        momentum, orbital, step_rows(step), part, :
                    ]
        return carry

    def shape_mate(slot, step):
        band = step // per_band
        for orbital in range(2):
            real = mate_raw[slot, orbital, step_rows(step), 0, :]
            imaginary = mate_raw[slot, orbital, step_rows(step), 1, :]
            first = orbital * 2 * BAND + lax.rem(step, per_band) * STEP
            plain = pl.ds(pl.multiple_of(first, STEP), STEP)
            turned = pl.ds(pl.multiple_of(first + BAND, STEP), STEP)
            mate[slot, band, plain, pl.ds(0, auxiliary)] = real
            mate[slot, band, plain, pl.ds(auxiliary, auxiliary)] = imaginary
            mate[slot, band, turned, pl.ds(0, auxiliary)] = -imaginary
            mate[slot, band, turned, pl.ds(auxiliary, auxiliary)] = real

    def shape_energies():
        sums = [occupied_ref[0] + occupied_ref[0], occupied_ref[0] + occupied_ref[1]]
        sums.append(occupied_ref[1] + occupied_ref[1])
        diagonal = lax.broadcasted_iota(
            jnp.int32, (virtuals, virtuals), 0
        ) == lax.broadcasted_iota(jnp.int32, (virtuals, virtuals), 1)
        mine = energy_ref[...].astype(jnp.float32)
        for momentum in range(2):
            spread = jnp.where(diagonal, mine[momentum : momentum + 1, :], 0.0)
            column = jnp.sum(spread, axis=1, keepdims=True)
            energy_left[momentum] = jnp.broadcast_to(column, (virtuals, LANES))
        energy_near(False).wait_recv()
        for slot in range(2):
            theirs = energy_in[slot].astype(jnp.float32)
            theirs = jnp.where(core == 0, theirs[0:1, :], theirs[1:2, :])
            for band in range(bands):
                part = theirs[:, band * BAND : (band + 1) * BAND]
                row = jnp.concatenate([part, part], axis=1)
                base = energy_left[chosen[slot]] + row
                for kind in range(3):
                    inverse[slot, band, kind] = 1.0 / (base - sums[kind])

    sign = jnp.where(lax.broadcasted_iota(jnp.int32, (virtuals, LANES), 1) < BAND, -1.0, 1.0)

    def add_band(slot, band):
        momentum = jnp.where(slot == 1, chosen[1], chosen[0])
        products[...] = lax.dot_general(
            own[momentum], mate[slot, band], (((1,), (1,)), ((), ())),
            preferred_element_type=jnp.float32,
        )
        amplitudes = {}
        for i in range(2):
            for j in range(2):
                value = products[i * virtuals : (i + 1) * virtuals, j * LANES : (j + 1) * LANES]
                amplitudes[i, j] = value * inverse[slot, band, i + j]
        combined, rounded, turned = [], [], []
        for i in range(2):
            for j in range(2):
                this = amplitudes[i, j]
                combined.append((2.0 * this - amplitudes[j, i]).astype(jnp.bfloat16))
                rounded.append(this.astype(jnp.bfloat16))
                turned.append((pltpu.roll(this, BAND, 1) * sign).astype(jnp.bfloat16))
        left = jnp.concatenate(combined, axis=1)
        right = jnp.concatenate(
            [jnp.concatenate(rounded, axis=1), jnp.concatenate(turned, axis=1)], axis=0
        )
        total[slot] += lax.dot_general(
            left, right, (((1,), (1,)), ((), ())), preferred_element_type=jnp.float32
        )

    def far_step(step):
        for piece in range(per_step):
            forward(step * per_step + piece)
        shape_mate(1, step)

    def near_step(step):
        for piece in range(per_step):
            near_copy(step * per_step + piece, False).wait_recv()
        shape_mate(0, step)

    total[...] = jnp.zeros_like(total)
    lax.fori_loop(0, steps // 2, shape_own, 0)
    far_step(0)
    energy_far().wait_recv()

    @pl.when(odd == 1)
    def _():
        energy_near(True).start()

    lax.fori_loop(steps // 2, steps, shape_own, 0)
    far_step(1)
    shape_energies()

    def main_step(step, carry):
        @pl.when(step > 1)
        def _():
            far_step(step)

        near_step(step - 1)
        phase = lax.rem(step, per_band)
        ready = jnp.logical_and(step >= per_band, jnp.logical_or(phase == 1, phase == 2))

        @pl.when(ready)
        def _():
            add_band(2 - phase, step // per_band - 1)

        return carry

    lax.fori_loop(1, steps, main_step, 0)

    def swap_copy(slot):
        return pltpu.make_async_remote_copy(
            src_ref=total.at[slot, pl.ds(pl.multiple_of(other * half, half), half), :],
            dst_ref=incoming.at[slot],
            send_sem=swap_send.at[slot], recv_sem=swap_recv.at[slot],
            device_id=(me, other), device_id_type=mesh_id,
        )

    add_band(1, bands - 1)
    swap_copy(1).start()
    near_step(steps - 1)
    add_band(0, bands - 1)
    swap_copy(0).start()

    def drain(piece, carry):
        far_copy(piece).wait_send()
        near_copy(piece, False).wait_send()
        return carry

    lax.fori_loop(0, pieces, drain, 0)
    energy_far().wait_send()
    energy_near(False).wait_send()
    here = pl.ds(pl.multiple_of(core * half, half), half)
    swap_copy(1).wait()
    for momentum in range(2):
        known = jnp.where(chosen[1] == momentum, total[1, here, :], incoming[1])
        partial[momentum] = known + jnp.where(chosen[0] == momentum, total[0, here, :], 0.0)
    swap_copy(0).wait()
    for momentum in range(2):
        value = partial[momentum] + jnp.where(chosen[0] == momentum, 0.0, incoming[0])
        for part in range(2):
            out_ref[momentum, :, part, :] = value[:, part * virtuals : (part + 1) * virtuals]


def fused(factors, occupied_energy, virtual_energy, conserve, pair_lists):
    momenta, orbitals, virtuals, parts, auxiliary = factors.shape
    ring = lax.axis_size("ka")
    pieces = virtuals // PIECE
    bands = virtuals // BAND
    dma = pltpu.SemaphoreType.DMA
    return pl.pallas_call(
        functools.partial(fused_kernel, ring, virtuals, auxiliary),
        out_shape=pltpu.VMEM((momenta, virtuals // 2, 2, virtuals), jnp.float32),
        in_specs=[
            pl.BlockSpec(memory_space=pltpu.HBM),
            pl.BlockSpec(memory_space=pltpu.HBM),
            pl.BlockSpec(memory_space=pltpu.HBM),
            pl.BlockSpec(memory_space=pltpu.HBM),
        ],
        out_specs=pl.BlockSpec(memory_space=pltpu.VMEM),
        scratch_shapes=[
            pltpu.SMEM(conserve.shape, conserve.dtype),
            pltpu.SMEM(occupied_energy.shape, occupied_energy.dtype),
            pltpu.VMEM(virtual_energy.shape, virtual_energy.dtype),
            pltpu.VMEM((momenta, orbitals, virtuals, parts, auxiliary), jnp.bfloat16),
            pltpu.VMEM((2, orbitals, virtuals, parts, auxiliary), jnp.bfloat16),
            pltpu.VMEM((momenta, orbitals * virtuals, parts * auxiliary), jnp.bfloat16),
            pltpu.VMEM((2, bands, orbitals * 2 * BAND, parts * auxiliary), jnp.bfloat16),
            pltpu.VMEM((2, momenta, virtuals), jnp.bfloat16),
            pltpu.VMEM((momenta, virtuals, LANES), jnp.float32),
            pltpu.VMEM((2, bands, 3, virtuals, LANES), jnp.float32),
            pltpu.VMEM((orbitals * virtuals, orbitals * 2 * BAND), jnp.float32),
            pltpu.VMEM((2, virtuals, 2 * virtuals), jnp.float32),
            pltpu.VMEM((2, virtuals // 2, 2 * virtuals), jnp.float32),
            pltpu.VMEM((2, virtuals // 2, 2 * virtuals), jnp.float32),
            dma((3,)), dma((2,)),
            dma((pieces,)), dma((pieces,)), dma((pieces,)), dma((pieces,)),
            dma((2,)), dma((2,)), dma((2,)), dma((2,)),
        ],
        compiler_params=pltpu.CompilerParams(
            collective_id=0, has_side_effects=True, vmem_limit_bytes=54 * 1024 * 1024
        ),
        name="density",
    )(conserve, occupied_energy, virtual_energy, factors)


def local(factors, occupied_energy, virtual_energy, conserve, pair_lists):
    momenta, orbitals, virtuals, parts, auxiliary = factors.shape
    rounds, pairs = pair_lists.shape[:2]
    ring, holders = lax.axis_size("ka"), lax.axis_size("occ")
    whole_square = pairs * holders == orbitals * orbitals
    fits = momenta == 2 and orbitals == 2 and holders == 2 and rounds == 2
    even = ring % 2 == 0 and ring > 4 and virtuals % BAND == 0 and auxiliary % LANES == 0
    chosen = fused if whole_square and fits and even else general
    return chosen(factors, occupied_energy, virtual_energy, conserve, pair_lists)


def solution(mesh):
    in_specs = (
        P("ka", None, None, None, None),
        P(),
        P("ka", None),
        P("ka", None),
        P(None, "occ", None),
    )
    out_specs = P("ka", "occ", None, None)
    return jax.shard_map(local, mesh=mesh, in_specs=in_specs, out_specs=out_specs, check_vma=False)
```
